256 devices in a mesh: gx: 16 (over z, core), gy: 4 (over x), gz: 4 (over y).
Axes of the slice: x: 4, y: 4, z: 8, core: 2. Of those that a mesh axis runs over, the one named last changes fastest.
Arguments:
- velocity: float32 [3, 1024, 128, 512], P(None, 'gx', 'gz', 'gy'), may hold values from -6 to 6
- tile_turbine: int32 [16, 4, 4, 2], P('gx', 'gz', 'gy'), may hold values from 0 to 63
- tile_plane: int32 [16, 4, 4, 2], P('gx', 'gz', 'gy'), may hold values from 0 to 63
- tile_weight: bfloat16 [16, 4, 4, 2, 384, 4096], P('gx', 'gz', 'gy'), may hold values from -0.09375 to 0.09375
- chord: float32 [64, 384], replicated, may hold values from 0.25 to 1
Outputs:
- predicted: float32 [3, 1024, 128, 512], P(None, 'gx', 'gz', 'gy')
- forces: float32 [64, 1152], replicated
The draws below stay inside these ranges and needn't reach their ends.
All inputs are finite; a program needn't handle non-finite values.
Results may differ from the reference program's by a relative error of at most 0.0032.
Values sent between devices are 32-bit elements; how exact they have to be, the bound alone decides.
No kernel may reach another device: no remote copies, remote signals or barrier semaphores. Data moves between devices by JAX's collectives and lax.ppermute only.
A program may use at most 128 MiB of HBM per device.

```python
import math
import jax
import jax.numpy as jnp
from jax import lax

CX = 64
PTS = 384
SLOTS = 2
TURB = 64
TILE = 4096
NX = 1024
NZ = 128
NY = 512
N_GX = 16
N_GY = 4
N_GZ = 4


def plant(array, stream_key, smallest, top_value):
    shape = array.shape
    place = [jax.random.randint(jax.random.fold_in(stream_key, axis), (), 0, shape[axis]) for axis in range(len(shape))]
    array = array.at[tuple(place)].set(smallest)
    longest = shape.index(max(shape))
    place[longest] = (place[longest] + 1) % shape[longest]
    return array.at[tuple(place)].set(top_value)


def level_of(key, dims, cuts, smallest, largest):
    level, own = 1.0, jax.random.fold_in(key, 6)
    for dim, blocks in cuts:
        draws = jnp.exp(jax.random.uniform(jax.random.fold_in(own, dim), (blocks,), jnp.float32, smallest / len(cuts), largest / len(cuts)))
        level = level * jnp.repeat(draws, dims[dim] // blocks).reshape([-1 if axis == dim else 1 for axis in range(len(dims))])
    return level


def centred(rng, dims, scale, bound, cuts=(), kind=jnp.bfloat16):
    level = level_of(rng, dims, cuts, -0.22, 0.18) if cuts else 1.0
    array = jax.random.normal(rng, dims, jnp.float32) * scale * level
    return jnp.minimum(jnp.maximum(array, -bound), bound).astype(kind)


def setup_inputs(seed: int = 0) -> dict:
    arg_keys = jax.random.split(jax.random.key(seed), 6)
    velocity = centred(arg_keys[0], (3, NX, NZ, NY), 1.0, 6.0, ((1, 16), (2, 4), (3, 4)), jnp.float32)
    tile_turbine = plant(jax.random.randint(arg_keys[1], (N_GX, N_GZ, N_GY, SLOTS), 0, TURB), jax.random.fold_in(arg_keys[1], 1), 0, TURB - 1).astype(jnp.int32)
    tile_plane = plant(jax.random.randint(arg_keys[2], (N_GX, N_GZ, N_GY, SLOTS), 0, CX), jax.random.fold_in(arg_keys[2], 1), 0, CX - 1).astype(jnp.int32)
    tile_weight = centred(arg_keys[3], (N_GX, N_GZ, N_GY, SLOTS, PTS, TILE), TILE ** -0.5, 0.09375, ((0, 16), (1, 4), (2, 4)))
    chord = jnp.clip(jnp.exp(jax.random.uniform(arg_keys[4], (TURB, PTS), jnp.float32, math.log(0.25), math.log(1.0))), 0.25, 1.0)
    return dict(velocity=velocity, tile_turbine=tile_turbine, tile_plane=tile_plane, tile_weight=tile_weight, chord=chord)


DIRS = (-3, -1, -2)

def shifted(p, axis, step):
    idx = [slice(1, -1), slice(1, -1), slice(1, -1)]
    idx[axis + 3] = slice(1 + step, p.shape[axis] - 1 + step)
    lead = [slice(None)] * (p.ndim - 3)
    return p[tuple(lead + idx)]

def strain_viscosity(p):
    grads = [[0.5 * (shifted(p[c], DIRS[d], 1) - shifted(p[c], DIRS[d], -1)) for d in range(3)] for c in range(3)]
    total = jnp.zeros_like(grads[0][0])
    for c in range(3):
        for d in range(3):
            strain = 0.5 * (grads[c][d] + grads[d][c])
            total = total + strain * strain
    return 0.05 + 1.0 * jnp.sqrt(2.0 * total + 1e-06)

def advance(padded, nu_padded):
    nu_here = shifted(nu_padded, -1, 0)
    result = []
    for c in range(3):
        center = shifted(padded[c], -1, 0)
        advect = jnp.zeros_like(center)
        spread = jnp.zeros_like(center)
        for d in range(3):
            upper = shifted(padded[c], DIRS[d], 1)
            lower = shifted(padded[c], DIRS[d], -1)
            advect = advect + shifted(padded[d], -1, 0) * 0.5 * (upper - lower)
            nu_up = 0.5 * (nu_here + shifted(nu_padded, DIRS[d], 1))
            nu_low = 0.5 * (nu_here + shifted(nu_padded, DIRS[d], -1))
            spread = spread + nu_up * (upper - center) - nu_low * (center - lower)
        result.append(center + 0.25 * (spread - advect))
    return jnp.stack(result)

def actuate(velocity_probe, coef):
    rows = velocity_probe.shape[0]
    parts = velocity_probe.reshape(rows, 3, -1)
    magnitude = jnp.sqrt(lax.optimization_barrier(jnp.sum(parts * parts, axis=1)) + 1e-06)
    return (-2.0 * coef[:, None, :] * magnitude[:, None, :] * parts).reshape(rows, -1)

def reference(velocity, tile_turbine, tile_plane, tile_weight, chord):
    grid_cells_x, grid_cells_z, grid_cells_y, tile_count = tile_turbine.shape
    cx = NX // grid_cells_x
    vertical_coord = NZ // grid_cells_z
    spanwise_coord = NY // grid_cells_y
    block_count = grid_cells_x * grid_cells_z * grid_cells_y
    actuator_count = tile_weight.shape[4]
    nturb = chord.shape[0]
    blocks = velocity.reshape(3, grid_cells_x, cx, grid_cells_z, vertical_coord, grid_cells_y, spanwise_coord).transpose(1, 3, 5, 0, 2, 4, 6).reshape(block_count, 3, cx, vertical_coord * spanwise_coord)
    turbine_list = tile_turbine.reshape(block_count, tile_count)
    rotor_planes = tile_plane.reshape(block_count, tile_count)
    spread_weights = tile_weight.reshape(block_count, tile_count, actuator_count, vertical_coord * spanwise_coord)
    picks = (rotor_planes[:, :, None] == jnp.arange(cx, dtype=jnp.int32)[None, None, :]).astype(jnp.float32)

    def sample_block(tile_index):
        tiles = jnp.einsum('sx,cxq->scq', picks[tile_index], blocks[tile_index], precision=lax.Precision.HIGHEST).astype(jnp.bfloat16)
        return jnp.einsum('spq,scq->scp', spread_weights[tile_index].astype(jnp.float32), tiles.astype(jnp.float32), precision=lax.Precision.HIGHEST)
    block_local = lax.map(sample_block, jnp.arange(block_count))
    owning_block = (turbine_list[:, :, None] == jnp.arange(nturb, dtype=jnp.int32)[None, None, :]).astype(jnp.float32)
    velocity_probe = jnp.einsum('ezf,ezw->fw', owning_block, block_local.reshape(block_count, tile_count, -1), precision=lax.Precision.HIGHEST)
    forces = actuate(velocity_probe, chord)
    tile_force = jnp.einsum('bst,tk->bsk', owning_block, forces, precision=lax.Precision.HIGHEST).astype(jnp.bfloat16)

    def spread_block(tile_index):
        forces_sent = jnp.einsum('axz,ahx->ahz', spread_weights[tile_index].astype(jnp.float32), tile_force[tile_index].reshape(tile_count, 3, actuator_count).astype(jnp.float32), precision=lax.Precision.HIGHEST)
        return jnp.einsum('sx,scq->cxq', picks[tile_index], forces_sent, precision=lax.Precision.HIGHEST)
    forces_sent = lax.map(spread_block, jnp.arange(block_count))
    impulse = forces_sent.reshape(grid_cells_x, grid_cells_z, grid_cells_y, 3, cx, vertical_coord, spanwise_coord).transpose(3, 0, 4, 1, 5, 2, 6).reshape(3, NX, NZ, NY)
    padded = jnp.pad(velocity, ((0, 0), (1, 1), (1, 1), (1, 1)))
    viscosity = strain_viscosity(padded)
    nu_padded = jnp.pad(viscosity, 1)
    predicted = advance(padded, nu_padded) + impulse
    return (predicted, forces)
```

```python
import jax
import jax.numpy as jnp
from jax import lax
from jax.sharding import PartitionSpec as P

DIRS = (-3, -1, -2)


def padded_2(block, sides, width):
    for axis, dim in sides:
        count = lax.axis_size(axis)
        forward = [(i, i + 1) for i in range(count - 1)]
        backward = [(target, source) for source, target in forward]
        low = lax.ppermute(
            lax.slice_in_dim(block, block.shape[dim] - width, None, axis=dim), axis, forward
        )
        high = lax.ppermute(lax.slice_in_dim(block, 0, width, axis=dim), axis, backward)
        block = jnp.concatenate([low, block, high], axis=dim)
    return block


def shifted(p, axis, step):
    idx = [slice(1, -1), slice(1, -1), slice(1, -1)]
    idx[axis + 3] = slice(1 + step, p.shape[axis] - 1 + step)
    lead = [slice(None)] * (p.ndim - 3)
    return p[tuple(lead + idx)]


def strain_viscosity(p):
    grads = [
        [0.5 * (shifted(p[c], DIRS[d], 1) - shifted(p[c], DIRS[d], -1)) for d in range(3)]
        for c in range(3)
    ]
    total = jnp.zeros_like(grads[0][0])
    for c in range(3):
        for d in range(3):
            strain = 0.5 * (grads[c][d] + grads[d][c])
            total = total + strain * strain
    return 0.05 + 1.0 * jnp.sqrt(2.0 * total + 1e-06)


def advance(padded, nu_padded):
    nu_here = shifted(nu_padded, -1, 0)
    result = []
    for c in range(3):
        center = shifted(padded[c], -1, 0)
        advect = jnp.zeros_like(center)
        spread = jnp.zeros_like(center)
        for d in range(3):
            upper = shifted(padded[c], DIRS[d], 1)
            lower = shifted(padded[c], DIRS[d], -1)
            advect = advect + shifted(padded[d], -1, 0) * 0.5 * (upper - lower)
            nu_up = 0.5 * (nu_here + shifted(nu_padded, DIRS[d], 1))
            nu_low = 0.5 * (nu_here + shifted(nu_padded, DIRS[d], -1))
            spread = spread + nu_up * (upper - center) - nu_low * (center - lower)
        result.append(center + 0.25 * (spread - advect))
    return jnp.stack(result)


def actuate(velocity_probe, coef):
    rows = velocity_probe.shape[0]
    parts = velocity_probe.reshape(rows, 3, -1)
    magnitude = jnp.sqrt(jnp.sum(parts * parts, axis=1) + 1e-06)
    return (-2.0 * coef[:, None, :] * magnitude[:, None, :] * parts).reshape(rows, -1)


def body(velocity, tile_turbine, tile_plane, tile_weight, chord):
    cx = velocity.shape[1]
    vertical_coord = velocity.shape[2]
    spanwise_coord = velocity.shape[3]
    tile_count = tile_turbine.shape[3]
    actuator_count = tile_weight.shape[4]
    nturb = chord.shape[0]
    turbine_list = tile_turbine.reshape(tile_count)
    rotor_planes = tile_plane.reshape(tile_count)
    spread_weights = tile_weight.reshape(
        tile_count, actuator_count, vertical_coord * spanwise_coord
    )
    flat = velocity.reshape(3, cx, vertical_coord * spanwise_coord)
    picks = (rotor_planes[:, None] == jnp.arange(cx, dtype=jnp.int32)[None, :]).astype(jnp.float32)
    tiles = jnp.einsum("sx,cxq->scq", picks, flat, precision=lax.Precision.HIGHEST).astype(
        jnp.bfloat16
    )
    block_local = jnp.einsum(
        "spq,scq->scp", spread_weights, tiles, preferred_element_type=jnp.float32
    )
    owning_block = (turbine_list[:, None] == jnp.arange(nturb, dtype=jnp.int32)[None, :]).astype(
        jnp.float32
    )
    partial_sample = jnp.einsum(
        "yr,yw->rw",
        owning_block,
        block_local.reshape(tile_count, -1),
        precision=lax.Precision.HIGHEST,
    )
    sample = lax.psum(partial_sample, ("gx", "gy", "gz"))
    forces = actuate(sample, chord)
    tile_force = jnp.dot(owning_block, forces, precision=lax.Precision.HIGHEST).astype(jnp.bfloat16)
    forces_sent = jnp.einsum(
        "axz,ahx->ahz",
        spread_weights,
        tile_force.reshape(tile_count, 3, actuator_count),
        preferred_element_type=jnp.float32,
    )
    impulse = jnp.einsum(
        "sx,scq->cxq", picks, forces_sent, precision=lax.Precision.HIGHEST
    ).reshape(3, cx, vertical_coord, spanwise_coord)
    padded = padded_2(velocity, (("gx", 1), ("gy", 3), ("gz", 2)), 1)
    viscosity = strain_viscosity(padded)
    nu_padded = padded_2(viscosity, (("gx", 0), ("gy", 2), ("gz", 1)), 1)
    predicted = advance(padded, nu_padded) + impulse
    return (predicted, forces)


def solution(mesh):
    placed = (
        P(None, "gx", "gz", "gy"),
        P("gx", "gz", "gy", None),
        P("gx", "gz", "gy", None),
        P("gx", "gz", "gy", None, None, None),
        P(),
    )
    return jax.shard_map(
        body,
        mesh=mesh,
        in_specs=placed,
        out_specs=(P(None, "gx", "gz", "gy"), P()),
        check_vma=False,
    )
```

```python
import jax
import jax.numpy as jnp
from jax import lax
from jax.sharding import PartitionSpec as P

DIRS = (-3, -1, -2)


def padded_2(block, sides, width):
    for axis, dim in sides:
        count = lax.axis_size(axis)
        forward = [(i, i + 1) for i in range(count - 1)]
        backward = [(target, source) for source, target in forward]
        low = lax.ppermute(
            lax.slice_in_dim(block, block.shape[dim] - width, None, axis=dim), axis, forward
        )
        high = lax.ppermute(lax.slice_in_dim(block, 0, width, axis=dim), axis, backward)
        block = jnp.concatenate([low, block, high], axis=dim)
    return block


def shifted(p, axis, step):
    idx = [slice(1, -1), slice(1, -1), slice(1, -1)]
    idx[axis + 3] = slice(1 + step, p.shape[axis] - 1 + step)
    lead = [slice(None)] * (p.ndim - 3)
    return p[tuple(lead + idx)]


def strain_viscosity(p):
    grads = [
        [0.5 * (shifted(p[c], DIRS[d], 1) - shifted(p[c], DIRS[d], -1)) for d in range(3)]
        for c in range(3)
    ]
    total = jnp.zeros_like(grads[0][0])
    for c in range(3):
        for d in range(3):
            strain = 0.5 * (grads[c][d] + grads[d][c])
            total = total + strain * strain
    return 0.05 + 1.0 * jnp.sqrt(2.0 * total + 1e-06)


def advance(padded, nu_padded):
    nu_here = shifted(nu_padded, -1, 0)
    result = []
    for c in range(3):
        center = shifted(padded[c], -1, 0)
        advect = jnp.zeros_like(center)
        spread = jnp.zeros_like(center)
        for d in range(3):
            upper = shifted(padded[c], DIRS[d], 1)
            lower = shifted(padded[c], DIRS[d], -1)
            advect = advect + shifted(padded[d], -1, 0) * 0.5 * (upper - lower)
            nu_up = 0.5 * (nu_here + shifted(nu_padded, DIRS[d], 1))
            nu_low = 0.5 * (nu_here + shifted(nu_padded, DIRS[d], -1))
            spread = spread + nu_up * (upper - center) - nu_low * (center - lower)
        result.append(center + 0.25 * (spread - advect))
    return jnp.stack(result)


def actuate(velocity_probe, coef):
    rows = velocity_probe.shape[0]
    parts = velocity_probe.reshape(rows, 3, -1)
    magnitude = jnp.sqrt(jnp.sum(parts * parts, axis=1) + 1e-06)
    return (-2.0 * coef[:, None, :] * magnitude[:, None, :] * parts).reshape(rows, -1)


def body(velocity, tile_turbine, tile_plane, tile_weight, chord):
    cx = velocity.shape[1]
    vertical_coord = velocity.shape[2]
    spanwise_coord = velocity.shape[3]
    tile_count = tile_turbine.shape[3]
    actuator_count = tile_weight.shape[4]
    nturb = chord.shape[0]
    turbine_list = tile_turbine.reshape(tile_count)
    rotor_planes = tile_plane.reshape(tile_count)
    spread_weights = tile_weight.reshape(
        tile_count, actuator_count, vertical_coord * spanwise_coord
    )
    flat = velocity.reshape(3, cx, vertical_coord * spanwise_coord)
    picks = (rotor_planes[:, None] == jnp.arange(cx, dtype=jnp.int32)[None, :]).astype(jnp.float32)
    tiles = jnp.einsum("sx,cxq->scq", picks, flat, precision=lax.Precision.HIGHEST).astype(
        jnp.bfloat16
    )
    block_local = jnp.einsum(
        "spq,scq->scp", spread_weights, tiles, preferred_element_type=jnp.float32
    )
    owning_block = (turbine_list[:, None] == jnp.arange(nturb, dtype=jnp.int32)[None, :]).astype(
        jnp.float32
    )
    partial_sample = jnp.einsum(
        "yr,yw->rw",
        owning_block,
        block_local.reshape(tile_count, -1),
        precision=lax.Precision.HIGHEST,
    )
    rows = lax.axis_size("gx")
    per_row = nturb // rows
    received = lax.all_to_all(
        partial_sample.reshape(rows, per_row, -1), "gx", split_axis=0, concat_axis=0, tiled=True
    )
    owned = jnp.sum(received, axis=0)
    for axis in ("gy", "gz"):
        count = lax.axis_size(axis)
        step = 1
        while step < count:
            pairs = [(i, i ^ step) for i in range(count)]
            owned = owned + lax.ppermute(owned, axis, pairs)
            step *= 2
    owned_coef = lax.dynamic_slice_in_dim(chord, lax.axis_index("gx") * per_row, per_row, 0)
    owned_force = actuate(owned, owned_coef)
    forces = lax.all_to_all(
        jnp.broadcast_to(owned_force[None], (rows,) + owned_force.shape),
        "gx", split_axis=0, concat_axis=0, tiled=True,
    ).reshape(nturb, -1)
    tile_force = jnp.dot(owning_block, forces, precision=lax.Precision.HIGHEST).astype(jnp.bfloat16)
    forces_sent = jnp.einsum(
        "axz,ahx->ahz",
        spread_weights,
        tile_force.reshape(tile_count, 3, actuator_count),
        preferred_element_type=jnp.float32,
    )
    impulse = jnp.einsum(
        "sx,scq->cxq", picks, forces_sent, precision=lax.Precision.HIGHEST
    ).reshape(3, cx, vertical_coord, spanwise_coord)
    padded = padded_2(velocity, (("gx", 1), ("gy", 3), ("gz", 2)), 1)
    viscosity = strain_viscosity(padded)
    nu_padded = padded_2(viscosity, (("gx", 0), ("gy", 2), ("gz", 1)), 1)
    predicted = advance(padded, nu_padded) + impulse
    return (predicted, forces)


def solution(mesh):
    placed = (
        P(None, "gx", "gz", "gy"),
        P("gx", "gz", "gy", None),
        P("gx", "gz", "gy", None),
        P("gx", "gz", "gy", None, None, None),
        P(),
    )
    return jax.shard_map(
        body,
        mesh=mesh,
        in_specs=placed,
        out_specs=(P(None, "gx", "gz", "gy"), P()),
        check_vma=False,
    )
```

```python
import jax
import jax.numpy as jnp
from jax import lax
from jax.experimental import pallas as pl
from jax.experimental.pallas import tpu as pltpu
from jax.sharding import PartitionSpec as P

INTERPRET = False


def actuate(velocity_probe, coef):
    rows = velocity_probe.shape[0]
    parts = velocity_probe.reshape(rows, 3, -1)
    magnitude = jnp.sqrt(jnp.sum(parts * parts, axis=1) + 1e-06)
    return (-2.0 * coef[:, None, :] * magnitude[:, None, :] * parts).reshape(rows, -1)


def faces(block, lead):
    out = []
    for axis, dim in (("gx", lead), ("gz", lead + 1), ("gy", lead + 2)):
        count = lax.axis_size(axis)
        forward = [(i, i + 1) for i in range(count - 1)]
        backward = [(target, source) for source, target in forward]
        size = block.shape[dim]
        low = lax.ppermute(lax.index_in_dim(block, size - 1, dim, keepdims=False), axis, forward)
        high = lax.ppermute(lax.index_in_dim(block, 0, dim, keepdims=False), axis, backward)
        if axis == "gy":
            low = jnp.swapaxes(low, -1, -2)
            high = jnp.swapaxes(high, -1, -2)
        out += [low, high]
    return out


def neighbours(ref, xlo, xhi, zlo, zhi, ylo, yhi, lead, x, centre):
    nx = ref.shape[-3]
    nz, ny = centre.shape
    sub = lax.broadcasted_iota(jnp.int32, (nz, ny), 0)
    lane = lax.broadcasted_iota(jnp.int32, (nz, ny), 1)
    column = lax.broadcasted_iota(jnp.int32, (nz, nx), 1)
    prev = ref[lead + (jnp.maximum(x - 1, 0),)]
    nxt = ref[lead + (jnp.minimum(x + 1, nx - 1),)]
    xm = jnp.where(x == 0, xlo[lead], prev)
    xp = jnp.where(x == nx - 1, xhi[lead], nxt)
    zl = zlo[lead + (pl.ds(x, 1), slice(None))]
    zh = zhi[lead + (pl.ds(x, 1), slice(None))]
    zm = jnp.where(sub == 0, zl, pltpu.roll(centre, 1, 0))
    zp = jnp.where(sub == nz - 1, zh, pltpu.roll(centre, nz - 1, 0))
    yl = jnp.sum(jnp.where(column == x, ylo[lead], 0.0), axis=1, keepdims=True)
    yh = jnp.sum(jnp.where(column == x, yhi[lead], 0.0), axis=1, keepdims=True)
    ym = jnp.where(lane == 0, yl, pltpu.roll(centre, 1, 1))
    yp = jnp.where(lane == ny - 1, yh, pltpu.roll(centre, ny - 1, 1))
    return xm, xp, ym, yp, zm, zp


def viscosity_kernel(u, xlo, xhi, zlo, zhi, ylo, yhi, nu):
    def plane(x, carry):
        grads = []
        for c in range(3):
            xm, xp, ym, yp, zm, zp = neighbours(u, xlo, xhi, zlo, zhi, ylo, yhi, (c,), x, u[c, x])
            grads.append([0.5 * (xp - xm), 0.5 * (yp - ym), 0.5 * (zp - zm)])
        total = jnp.zeros_like(grads[0][0])
        for c in range(3):
            for d in range(3):
                strain = 0.5 * (grads[c][d] + grads[d][c])
                total = total + strain * strain
        nu[x] = 0.05 + 1.0 * jnp.sqrt(2.0 * total + 1e-06)
        return carry

    lax.fori_loop(0, u.shape[1], plane, 0)


def advance_kernel(planes, u, xlo, xhi, zlo, zhi, ylo, yhi, nu, nxlo, nxhi, nzlo, nzhi, nylo, nyhi, sent, out):
    slots = sent.shape[0]

    def plane(x, carry):
        here = nu[x]
        nxm, nxp, nym, nyp, nzm, nzp = neighbours(nu, nxlo, nxhi, nzlo, nzhi, nylo, nyhi, (), x, here)
        nu_up = [0.5 * (here + nxp), 0.5 * (here + nyp), 0.5 * (here + nzp)]
        nu_low = [0.5 * (here + nxm), 0.5 * (here + nym), 0.5 * (here + nzm)]
        centres = [u[c, x] for c in range(3)]
        for c in range(3):
            center = centres[c]
            xm, xp, ym, yp, zm, zp = neighbours(u, xlo, xhi, zlo, zhi, ylo, yhi, (c,), x, center)
            upper = (xp, yp, zp)
            lower = (xm, ym, zm)
            advect = jnp.zeros_like(center)
            spread = jnp.zeros_like(center)
            for d in range(3):
                advect = advect + centres[d] * 0.5 * (upper[d] - lower[d])
                spread = spread + nu_up[d] * (upper[d] - center) - nu_low[d] * (center - lower[d])
            impulse = jnp.zeros_like(center)
            for s in range(slots):
                impulse = impulse + jnp.where(planes[s] == x, sent[s, c], 0.0)
            out[c, x] = center + 0.25 * (spread - advect) + impulse
        return carry

    lax.fori_loop(0, u.shape[1], plane, 0)


def vmem_call(kernel, out_shape, count, smem=0):
    specs = [pl.BlockSpec(memory_space=pltpu.SMEM)] * smem
    specs += [pl.BlockSpec(memory_space=pltpu.VMEM)] * (count - smem)
    return pl.pallas_call(
        kernel,
        out_shape=out_shape,
        in_specs=specs,
        out_specs=pl.BlockSpec(memory_space=pltpu.VMEM),
        interpret=INTERPRET,
    )


def stencil(velocity, planes, sent):
    u_faces = faces(velocity, 1)
    nu = vmem_call(
        viscosity_kernel, jax.ShapeDtypeStruct(velocity.shape[1:], jnp.float32), 7
    )(velocity, *u_faces)
    nu_faces = faces(nu, 0)
    return vmem_call(
        advance_kernel, jax.ShapeDtypeStruct(velocity.shape, jnp.float32), 16, smem=1
    )(planes, velocity, *u_faces, nu, *nu_faces, sent)


def body(velocity, tile_turbine, tile_plane, tile_weight, chord):
    cx = velocity.shape[1]
    vertical_coord = velocity.shape[2]
    spanwise_coord = velocity.shape[3]
    tile_count = tile_turbine.shape[3]
    actuator_count = tile_weight.shape[4]
    nturb = chord.shape[0]
    turbine_list = tile_turbine.reshape(tile_count)
    rotor_planes = tile_plane.reshape(tile_count)
    spread_weights = tile_weight.reshape(
        tile_count, actuator_count, vertical_coord * spanwise_coord
    )
    flat = velocity.reshape(3, cx, vertical_coord * spanwise_coord)
    picks = (rotor_planes[:, None] == jnp.arange(cx, dtype=jnp.int32)[None, :]).astype(jnp.float32)
    tiles = jnp.einsum("sx,cxq->scq", picks, flat, precision=lax.Precision.HIGHEST).astype(
        jnp.bfloat16
    )
    block_local = jnp.einsum(
        "spq,scq->scp", spread_weights, tiles, preferred_element_type=jnp.float32
    )
    owning_block = (turbine_list[:, None] == jnp.arange(nturb, dtype=jnp.int32)[None, :]).astype(
        jnp.float32
    )
    partial_sample = jnp.einsum(
        "yr,yw->rw",
        owning_block,
        block_local.reshape(tile_count, -1),
        precision=lax.Precision.HIGHEST,
    )
    rows = lax.axis_size("gx")
    per_row = nturb // rows
    received = lax.all_to_all(
        partial_sample.reshape(rows, per_row, -1), "gx", split_axis=0, concat_axis=0, tiled=True
    )
    owned = jnp.sum(received, axis=0)
    for axis in ("gy", "gz"):
        count = lax.axis_size(axis)
        step = 1
        while step < count:
            pairs = [(i, i ^ step) for i in range(count)]
            owned = owned + lax.ppermute(owned, axis, pairs)
            step *= 2
    owned_coef = lax.dynamic_slice_in_dim(chord, lax.axis_index("gx") * per_row, per_row, 0)
    owned_force = actuate(owned, owned_coef)
    forces = lax.all_to_all(
        jnp.broadcast_to(owned_force[None], (rows,) + owned_force.shape),
        "gx", split_axis=0, concat_axis=0, tiled=True,
    ).reshape(nturb, -1)
    tile_force = jnp.dot(owning_block, forces, precision=lax.Precision.HIGHEST).astype(jnp.bfloat16)
    forces_sent = jnp.einsum(
        "axz,ahx->ahz",
        spread_weights,
        tile_force.reshape(tile_count, 3, actuator_count),
        preferred_element_type=jnp.float32,
    ).reshape(tile_count, 3, vertical_coord, spanwise_coord)
    predicted = stencil(velocity[:, :, :, :], rotor_planes, forces_sent)
    return (predicted, forces)


def solution(mesh):
    placed = (
        P(None, "gx", "gz", "gy"),
        P("gx", "gz", "gy", None),
        P("gx", "gz", "gy", None),
        P("gx", "gz", "gy", None, None, None),
        P(),
    )
    return jax.shard_map(
        body,
        mesh=mesh,
        in_specs=placed,
        out_specs=(P(None, "gx", "gz", "gy"), P()),
        check_vma=False,
    )
```

```python
import jax
import jax.numpy as jnp
from jax import lax
from jax.experimental import pallas as pl
from jax.experimental.pallas import tpu as pltpu
from jax.sharding import PartitionSpec as P

INTERPRET = False


def actuate(velocity_probe, coef):
    rows = velocity_probe.shape[0]
    parts = velocity_probe.reshape(rows, 3, -1)
    magnitude = jnp.sqrt(jnp.sum(parts * parts, axis=1) + 1e-06)
    return (-2.0 * coef[:, None, :] * magnitude[:, None, :] * parts).reshape(rows, -1)


def faces(block, lead):
    out = []
    for axis, dim in (("gx", lead), ("gz", lead + 1), ("gy", lead + 2)):
        count = lax.axis_size(axis)
        forward = [(i, i + 1) for i in range(count - 1)]
        backward = [(target, source) for source, target in forward]
        size = block.shape[dim]
        low = lax.ppermute(lax.index_in_dim(block, size - 1, dim, keepdims=False), axis, forward)
        high = lax.ppermute(lax.index_in_dim(block, 0, dim, keepdims=False), axis, backward)
        if axis == "gy":
            low = jnp.swapaxes(low, -1, -2)
            high = jnp.swapaxes(high, -1, -2)
        out += [low, high]
    return out


def neighbours(ref, xlo, xhi, zlo, zhi, ylo, yhi, lead, x, centre):
    nx = ref.shape[-3]
    nz, ny = centre.shape
    sub = lax.broadcasted_iota(jnp.int32, (nz, ny), 0)
    lane = lax.broadcasted_iota(jnp.int32, (nz, ny), 1)
    column = lax.broadcasted_iota(jnp.int32, (nz, nx), 1)
    prev = ref[lead + (jnp.maximum(x - 1, 0),)]
    nxt = ref[lead + (jnp.minimum(x + 1, nx - 1),)]
    xm = jnp.where(x == 0, xlo[lead], prev)
    xp = jnp.where(x == nx - 1, xhi[lead], nxt)
    zl = zlo[lead + (pl.ds(x, 1), slice(None))]
    zh = zhi[lead + (pl.ds(x, 1), slice(None))]
    zm = jnp.where(sub == 0, zl, pltpu.roll(centre, 1, 0))
    zp = jnp.where(sub == nz - 1, zh, pltpu.roll(centre, nz - 1, 0))
    yl = jnp.sum(jnp.where(column == x, ylo[lead], 0.0), axis=1, keepdims=True)
    yh = jnp.sum(jnp.where(column == x, yhi[lead], 0.0), axis=1, keepdims=True)
    ym = jnp.where(lane == 0, yl, pltpu.roll(centre, 1, 1))
    yp = jnp.where(lane == ny - 1, yh, pltpu.roll(centre, ny - 1, 1))
    return xm, xp, ym, yp, zm, zp


def viscosity_kernel(u, xlo, xhi, zlo, zhi, ylo, yhi, nu):
    def plane(x, carry):
        grads = []
        for c in range(3):
            xm, xp, ym, yp, zm, zp = neighbours(u, xlo, xhi, zlo, zhi, ylo, yhi, (c,), x, u[c, x])
            grads.append([0.5 * (xp - xm), 0.5 * (yp - ym), 0.5 * (zp - zm)])
        total = jnp.zeros_like(grads[0][0])
        for c in range(3):
            for d in range(3):
                strain = 0.5 * (grads[c][d] + grads[d][c])
                total = total + strain * strain
        nu[x] = 0.05 + 1.0 * jnp.sqrt(2.0 * total + 1e-06)
        return carry

    lax.fori_loop(0, u.shape[1], plane, 0)


def advance_kernel(planes, u, xlo, xhi, zlo, zhi, ylo, yhi, nu, nxlo, nxhi, nzlo, nzhi, nylo, nyhi, sent, out):
    slots = sent.shape[0]

    def plane(x, carry):
        here = nu[x]
        nxm, nxp, nym, nyp, nzm, nzp = neighbours(nu, nxlo, nxhi, nzlo, nzhi, nylo, nyhi, (), x, here)
        nu_up = [0.5 * (here + nxp), 0.5 * (here + nyp), 0.5 * (here + nzp)]
        nu_low = [0.5 * (here + nxm), 0.5 * (here + nym), 0.5 * (here + nzm)]
        centres = [u[c, x] for c in range(3)]
        for c in range(3):
            center = centres[c]
            xm, xp, ym, yp, zm, zp = neighbours(u, xlo, xhi, zlo, zhi, ylo, yhi, (c,), x, center)
            upper = (xp, yp, zp)
            lower = (xm, ym, zm)
            advect = jnp.zeros_like(center)
            spread = jnp.zeros_like(center)
            for d in range(3):
                advect = advect + centres[d] * 0.5 * (upper[d] - lower[d])
                spread = spread + nu_up[d] * (upper[d] - center) - nu_low[d] * (center - lower[d])
            impulse = jnp.zeros_like(center)
            for s in range(slots):
                impulse = impulse + jnp.where(planes[s] == x, sent[s, c], 0.0)
            out[c, x] = center + 0.25 * (spread - advect) + impulse
        return carry

    lax.fori_loop(0, u.shape[1], plane, 0)


def vmem_call(kernel, out_shape, count, smem=0):
    specs = [pl.BlockSpec(memory_space=pltpu.SMEM)] * smem
    specs += [pl.BlockSpec(memory_space=pltpu.VMEM)] * (count - smem)
    return pl.pallas_call(
        kernel,
        out_shape=out_shape,
        in_specs=specs,
        out_specs=pl.BlockSpec(memory_space=pltpu.VMEM),
        interpret=INTERPRET,
    )


def stencil(velocity, planes, sent):
    u_faces = faces(velocity, 1)
    nu = vmem_call(
        viscosity_kernel, jax.ShapeDtypeStruct(velocity.shape[1:], jnp.float32), 7
    )(velocity, *u_faces)
    nu_faces = faces(nu, 0)
    return vmem_call(
        advance_kernel, jax.ShapeDtypeStruct(velocity.shape, jnp.float32), 16, smem=1
    )(planes, velocity, *u_faces, nu, *nu_faces, sent)


def body(velocity, tile_turbine, tile_plane, tile_weight, chord):
    cx = velocity.shape[1]
    vertical_coord = velocity.shape[2]
    spanwise_coord = velocity.shape[3]
    tile_count = tile_turbine.shape[3]
    actuator_count = tile_weight.shape[4]
    nturb = chord.shape[0]
    turbine_list = tile_turbine.reshape(tile_count)
    rotor_planes = tile_plane.reshape(tile_count)
    spread_weights = tile_weight.reshape(
        tile_count, actuator_count, vertical_coord * spanwise_coord
    )
    flat = velocity.reshape(3, cx, vertical_coord * spanwise_coord)
    picks = (rotor_planes[:, None] == jnp.arange(cx, dtype=jnp.int32)[None, :]).astype(jnp.float32)
    tiles = jnp.einsum("sx,cxq->scq", picks, flat, precision=lax.Precision.HIGHEST).astype(
        jnp.bfloat16
    )
    block_local = jnp.einsum(
        "spq,scq->scp", spread_weights, tiles, preferred_element_type=jnp.float32
    )
    owning_block = (turbine_list[:, None] == jnp.arange(nturb, dtype=jnp.int32)[None, :]).astype(
        jnp.float32
    )
    partial_sample = jnp.einsum(
        "yr,yw->rw",
        owning_block,
        block_local.reshape(tile_count, -1),
        precision=lax.Precision.HIGHEST,
    )
    everyone = ("gx", "gy", "gz")
    devices = lax.axis_size(everyone)
    pieces = devices // nturb
    width = actuator_count // pieces
    scattered = (
        partial_sample.reshape(nturb, 3, pieces, width).transpose(0, 2, 1, 3).reshape(devices, -1)
    )
    received = lax.all_to_all(scattered, everyone, split_axis=0, concat_axis=0, tiled=True)
    owned = jnp.sum(received, axis=0).reshape(1, -1)
    owned_coef = lax.dynamic_slice_in_dim(
        chord.reshape(devices, width), lax.axis_index(everyone), 1, 0
    )
    owned_force = actuate(owned, owned_coef)
    forces = (
        lax.all_to_all(
            jnp.broadcast_to(owned_force, (devices, owned_force.shape[1])),
            everyone, split_axis=0, concat_axis=0, tiled=True,
        )
        .reshape(nturb, pieces, 3, width)
        .transpose(0, 2, 1, 3)
        .reshape(nturb, -1)
    )
    tile_force = jnp.dot(owning_block, forces, precision=lax.Precision.HIGHEST).astype(jnp.bfloat16)
    forces_sent = jnp.einsum(
        "axz,ahx->ahz",
        spread_weights,
        tile_force.reshape(tile_count, 3, actuator_count),
        preferred_element_type=jnp.float32,
    ).reshape(tile_count, 3, vertical_coord, spanwise_coord)
    predicted = stencil(velocity[:, :, :, :], rotor_planes, forces_sent)
    return (predicted, forces)


def solution(mesh):
    placed = (
        P(None, "gx", "gz", "gy"),
        P("gx", "gz", "gy", None),
        P("gx", "gz", "gy", None),
        P("gx", "gz", "gy", None, None, None),
        P(),
    )
    return jax.shard_map(
        body,
        mesh=mesh,
        in_specs=placed,
        out_specs=(P(None, "gx", "gz", "gy"), P()),
        check_vma=False,
    )
```

```python
import jax
import jax.numpy as jnp
from jax import lax
from jax.experimental import pallas as pl
from jax.experimental.pallas import tpu as pltpu
from jax.sharding import PartitionSpec as P

INTERPRET = False


def actuate(velocity_probe, coef):
    rows = velocity_probe.shape[0]
    parts = velocity_probe.reshape(rows, 3, -1)
    magnitude = jnp.sqrt(jnp.sum(parts * parts, axis=1) + 1e-06)
    return (-2.0 * coef[:, None, :] * magnitude[:, None, :] * parts).reshape(rows, -1)


def exchange(first, last):
    out = []
    for axis, lo, hi in zip(("gx", "gz", "gy"), last, first):
        count = lax.axis_size(axis)
        forward = [(i, i + 1) for i in range(count - 1)]
        backward = [(target, source) for source, target in forward]
        out += [lax.ppermute(lo, axis, forward), lax.ppermute(hi, axis, backward)]
    return out


def keep_edges(plane, x, nz, ny, cols, rows_first, rows_last, lead):
    column = lax.broadcasted_iota(jnp.int32, cols[0].shape, 1)
    rows_first[lead + (pl.ds(x, 1), slice(None))] = plane[0:1, :]
    rows_last[lead + (pl.ds(x, 1), slice(None))] = plane[nz - 1 : nz, :]
    return (
        jnp.where(column == x, plane[:, 0:1], cols[0]),
        jnp.where(column == x, plane[:, ny - 1 : ny], cols[1]),
    )


def edges_kernel(u, zfirst, zlast, yfirst, ylast):
    nx, nz, ny = u.shape[1:]

    def plane(x, carry):
        out = []
        for c in range(3):
            out += keep_edges(u[c, x], x, nz, ny, carry[2 * c : 2 * c + 2], zfirst, zlast, (c,))
        return tuple(out)

    zero = jnp.zeros(yfirst.shape[1:], jnp.float32)
    cols = lax.fori_loop(0, nx, plane, (zero,) * 6)
    for c in range(3):
        yfirst[c] = cols[2 * c]
        ylast[c] = cols[2 * c + 1]


def neighbours(ref, xlo, xhi, zlo, zhi, ylo, yhi, lead, x, centre):
    nx = ref.shape[-3]
    nz, ny = centre.shape
    sub = lax.broadcasted_iota(jnp.int32, (nz, ny), 0)
    lane = lax.broadcasted_iota(jnp.int32, (nz, ny), 1)
    column = lax.broadcasted_iota(jnp.int32, (nz, nx), 1)
    prev = ref[lead + (jnp.maximum(x - 1, 0),)]
    nxt = ref[lead + (jnp.minimum(x + 1, nx - 1),)]
    xm = jnp.where(x == 0, xlo[lead], prev)
    xp = jnp.where(x == nx - 1, xhi[lead], nxt)
    zl = zlo[lead + (pl.ds(x, 1), slice(None))]
    zh = zhi[lead + (pl.ds(x, 1), slice(None))]
    zm = jnp.where(sub == 0, zl, pltpu.roll(centre, 1, 0))
    zp = jnp.where(sub == nz - 1, zh, pltpu.roll(centre, nz - 1, 0))
    yl = jnp.sum(jnp.where(column == x, ylo[lead], 0.0), axis=1, keepdims=True)
    yh = jnp.sum(jnp.where(column == x, yhi[lead], 0.0), axis=1, keepdims=True)
    ym = jnp.where(lane == 0, yl, pltpu.roll(centre, 1, 1))
    yp = jnp.where(lane == ny - 1, yh, pltpu.roll(centre, ny - 1, 1))
    return xm, xp, ym, yp, zm, zp


def viscosity_kernel(u, xlo, xhi, zlo, zhi, ylo, yhi, nu, zfirst, zlast, yfirst, ylast):
    nz, ny = u.shape[2:]

    def plane(x, carry):
        grads = []
        for c in range(3):
            xm, xp, ym, yp, zm, zp = neighbours(u, xlo, xhi, zlo, zhi, ylo, yhi, (c,), x, u[c, x])
            grads.append([0.5 * (xp - xm), 0.5 * (yp - ym), 0.5 * (zp - zm)])
        total = jnp.zeros_like(grads[0][0])
        for c in range(3):
            for d in range(3):
                strain = 0.5 * (grads[c][d] + grads[d][c])
                total = total + strain * strain
        here = 0.05 + 1.0 * jnp.sqrt(2.0 * total + 1e-06)
        nu[x] = here
        return keep_edges(here, x, nz, ny, carry, zfirst, zlast, ())

    zero = jnp.zeros(yfirst.shape, jnp.float32)
    yfirst[...], ylast[...] = lax.fori_loop(0, u.shape[1], plane, (zero, zero))


def advance_kernel(planes, u, xlo, xhi, zlo, zhi, ylo, yhi, nu, nxlo, nxhi, nzlo, nzhi, nylo, nyhi, sent, out):
    slots = sent.shape[0]

    def plane(x, carry):
        here = nu[x]
        nxm, nxp, nym, nyp, nzm, nzp = neighbours(nu, nxlo, nxhi, nzlo, nzhi, nylo, nyhi, (), x, here)
        nu_up = [0.5 * (here + nxp), 0.5 * (here + nyp), 0.5 * (here + nzp)]
        nu_low = [0.5 * (here + nxm), 0.5 * (here + nym), 0.5 * (here + nzm)]
        centres = [u[c, x] for c in range(3)]
        for c in range(3):
            center = centres[c]
            xm, xp, ym, yp, zm, zp = neighbours(u, xlo, xhi, zlo, zhi, ylo, yhi, (c,), x, center)
            upper = (xp, yp, zp)
            lower = (xm, ym, zm)
            advect = jnp.zeros_like(center)
            spread = jnp.zeros_like(center)
            for d in range(3):
                advect = advect + centres[d] * 0.5 * (upper[d] - lower[d])
                spread = spread + nu_up[d] * (upper[d] - center) - nu_low[d] * (center - lower[d])
            impulse = jnp.zeros_like(center)
            for s in range(slots):
                impulse = impulse + jnp.where(planes[s] == x, sent[s, c], 0.0)
            out[c, x] = center + 0.25 * (spread - advect) + impulse
        return carry

    lax.fori_loop(0, u.shape[1], plane, 0)


def vmem_call(kernel, out_shape, count, smem=0):
    specs = [pl.BlockSpec(memory_space=pltpu.SMEM)] * smem
    specs += [pl.BlockSpec(memory_space=pltpu.VMEM)] * (count - smem)
    return pl.pallas_call(
        kernel,
        out_shape=out_shape,
        in_specs=specs,
        out_specs=jax.tree.map(lambda _: pl.BlockSpec(memory_space=pltpu.VMEM), out_shape),
        interpret=INTERPRET,
    )


def stencil(velocity, planes, sent):
    nx, nz, ny = velocity.shape[1:]
    f32 = jnp.float32
    zfirst, zlast, yfirst, ylast = vmem_call(
        edges_kernel,
        (jax.ShapeDtypeStruct((3, nx, ny), f32),) * 2 + (jax.ShapeDtypeStruct((3, nz, nx), f32),) * 2,
        1,
    )(velocity)
    u_faces = exchange((velocity[:, 0], zfirst, yfirst), (velocity[:, nx - 1], zlast, ylast))
    nu, nzfirst, nzlast, nyfirst, nylast = vmem_call(
        viscosity_kernel,
        (jax.ShapeDtypeStruct((nx, nz, ny), f32),)
        + (jax.ShapeDtypeStruct((nx, ny), f32),) * 2
        + (jax.ShapeDtypeStruct((nz, nx), f32),) * 2,
        7,
    )(velocity, *u_faces)
    nu_faces = exchange((nu[0], nzfirst, nyfirst), (nu[nx - 1], nzlast, nylast))
    return vmem_call(
        advance_kernel, jax.ShapeDtypeStruct(velocity.shape, f32), 16, smem=1
    )(planes, velocity, *u_faces, nu, *nu_faces, sent)


def body(velocity, tile_turbine, tile_plane, tile_weight, chord):
    cx = velocity.shape[1]
    vertical_coord = velocity.shape[2]
    spanwise_coord = velocity.shape[3]
    tile_count = tile_turbine.shape[3]
    actuator_count = tile_weight.shape[4]
    nturb = chord.shape[0]
    turbine_list = tile_turbine.reshape(tile_count)
    rotor_planes = tile_plane.reshape(tile_count)
    spread_weights = tile_weight.reshape(
        tile_count, actuator_count, vertical_coord * spanwise_coord
    )
    tiles = jnp.stack(
        [lax.dynamic_index_in_dim(velocity, rotor_planes[s], 1, keepdims=False) for s in range(tile_count)]
    ).reshape(tile_count, 3, vertical_coord * spanwise_coord).astype(jnp.bfloat16)
    block_local = jnp.einsum(
        "spq,scq->scp", spread_weights, tiles, preferred_element_type=jnp.float32
    )
    owning_block = (turbine_list[:, None] == jnp.arange(nturb, dtype=jnp.int32)[None, :]).astype(
        jnp.float32
    )
    partial_sample = jnp.einsum(
        "yr,yw->rw",
        owning_block,
        block_local.reshape(tile_count, -1),
        precision=lax.Precision.HIGHEST,
    )
    rows = lax.axis_size("gx")
    per_row = nturb // rows
    received = lax.all_to_all(
        partial_sample.reshape(rows, per_row, -1), "gx", split_axis=0, concat_axis=0, tiled=True
    )
    owned = jnp.sum(received, axis=0)
    for axis in ("gy", "gz"):
        count = lax.axis_size(axis)
        step = 1
        while step < count:
            pairs = [(i, i ^ step) for i in range(count)]
            owned = owned + lax.ppermute(owned, axis, pairs)
            step *= 2
    owned_coef = lax.dynamic_slice_in_dim(chord, lax.axis_index("gx") * per_row, per_row, 0)
    owned_force = actuate(owned, owned_coef)
    forces = lax.all_to_all(
        jnp.broadcast_to(owned_force[None], (rows,) + owned_force.shape),
        "gx", split_axis=0, concat_axis=0, tiled=True,
    ).reshape(nturb, -1)
    tile_force = jnp.dot(owning_block, forces, precision=lax.Precision.HIGHEST).astype(jnp.bfloat16)
    forces_sent = jnp.einsum(
        "axz,ahx->ahz",
        spread_weights,
        tile_force.reshape(tile_count, 3, actuator_count),
        preferred_element_type=jnp.float32,
    ).reshape(tile_count, 3, vertical_coord, spanwise_coord)
    predicted = stencil(velocity[:, :, :, :], rotor_planes, forces_sent)
    return (predicted, forces)


def solution(mesh):
    placed = (
        P(None, "gx", "gz", "gy"),
        P("gx", "gz", "gy", None),
        P("gx", "gz", "gy", None),
        P("gx", "gz", "gy", None, None, None),
        P(),
    )
    return jax.shard_map(
        body,
        mesh=mesh,
        in_specs=placed,
        out_specs=(P(None, "gx", "gz", "gy"), P()),
        check_vma=False,
    )
```

```python
import jax
import jax.numpy as jnp
from jax import lax
from jax.experimental import pallas as pl
from jax.experimental.pallas import tpu as pltpu
from jax.sharding import PartitionSpec as P

INTERPRET = False


def actuate(velocity_probe, coef):
    rows = velocity_probe.shape[0]
    parts = velocity_probe.reshape(rows, 3, -1)
    magnitude = jnp.sqrt(jnp.sum(parts * parts, axis=1) + 1e-06)
    return (-2.0 * coef[:, None, :] * magnitude[:, None, :] * parts).reshape(rows, -1)


def faces(block, lead):
    out = []
    for axis, dim in (("gx", lead), ("gz", lead + 1), ("gy", lead + 2)):
        count = lax.axis_size(axis)
        forward = [(i, i + 1) for i in range(count - 1)]
        backward = [(target, source) for source, target in forward]
        size = block.shape[dim]
        low = lax.ppermute(lax.index_in_dim(block, size - 1, dim, keepdims=False), axis, forward)
        high = lax.ppermute(lax.index_in_dim(block, 0, dim, keepdims=False), axis, backward)
        if axis == "gy":
            low = jnp.swapaxes(low, -1, -2)
            high = jnp.swapaxes(high, -1, -2)
        out += [low, high]
    return out


def halo_columns(ycols, x):
    nx = ycols.shape[1]
    pick = (lax.broadcasted_iota(jnp.int32, (nx, 128), 0) == x).astype(jnp.float32)
    return jnp.dot(ycols[...], pick, precision=lax.Precision.HIGHEST, preferred_element_type=jnp.float32)


def neighbours(ref, xlo, xhi, zlo, zhi, yl, yh, lead, x, centre):
    nx = ref.shape[-3]
    nz, ny = centre.shape
    sub = lax.broadcasted_iota(jnp.int32, (nz, ny), 0)
    lane = lax.broadcasted_iota(jnp.int32, (nz, ny), 1)
    prev = ref[lead + (jnp.maximum(x - 1, 0),)]
    nxt = ref[lead + (jnp.minimum(x + 1, nx - 1),)]
    xm = jnp.where(x == 0, xlo[lead], prev)
    xp = jnp.where(x == nx - 1, xhi[lead], nxt)
    zl = zlo[lead + (pl.ds(x, 1), slice(None))]
    zh = zhi[lead + (pl.ds(x, 1), slice(None))]
    zm = jnp.where(sub == 0, zl, pltpu.roll(centre, 1, 0))
    zp = jnp.where(sub == nz - 1, zh, pltpu.roll(centre, nz - 1, 0))
    ym = jnp.where(lane == 0, yl, pltpu.roll(centre, 1, 1))
    yp = jnp.where(lane == ny - 1, yh, pltpu.roll(centre, ny - 1, 1))
    return xm, xp, ym, yp, zm, zp


def viscosity_kernel(u, xlo, xhi, zlo, zhi, ycols, nu):
    nz = u.shape[2]

    def plane(x, carry):
        cols = halo_columns(ycols, x)
        grads = []
        for c in range(3):
            yl = cols[nz * c : nz * (c + 1)]
            yh = cols[nz * (c + 3) : nz * (c + 4)]
            xm, xp, ym, yp, zm, zp = neighbours(u, xlo, xhi, zlo, zhi, yl, yh, (c,), x, u[c, x])
            grads.append([0.5 * (xp - xm), 0.5 * (yp - ym), 0.5 * (zp - zm)])
        total = jnp.zeros_like(grads[0][0])
        for c in range(3):
            for d in range(3):
                strain = 0.5 * (grads[c][d] + grads[d][c])
                total = total + strain * strain
        nu[x] = 0.05 + 1.0 * jnp.sqrt(2.0 * total + 1e-06)
        return carry

    lax.fori_loop(0, u.shape[1], plane, 0)


def advance_kernel(planes, u, xlo, xhi, zlo, zhi, nu, nxlo, nxhi, nzlo, nzhi, ycols, sent, out):
    slots = sent.shape[0]
    nz = u.shape[2]

    def plane(x, carry):
        cols = halo_columns(ycols, x)
        here = nu[x]
        nyl = cols[nz * 6 : nz * 7]
        nyh = cols[nz * 7 : nz * 8]
        nxm, nxp, nym, nyp, nzm, nzp = neighbours(nu, nxlo, nxhi, nzlo, nzhi, nyl, nyh, (), x, here)
        nu_up = [0.5 * (here + nxp), 0.5 * (here + nyp), 0.5 * (here + nzp)]
        nu_low = [0.5 * (here + nxm), 0.5 * (here + nym), 0.5 * (here + nzm)]
        centres = [u[c, x] for c in range(3)]
        for c in range(3):
            center = centres[c]
            yl = cols[nz * c : nz * (c + 1)]
            yh = cols[nz * (c + 3) : nz * (c + 4)]
            xm, xp, ym, yp, zm, zp = neighbours(u, xlo, xhi, zlo, zhi, yl, yh, (c,), x, center)
            upper = (xp, yp, zp)
            lower = (xm, ym, zm)
            advect = jnp.zeros_like(center)
            spread = jnp.zeros_like(center)
            for d in range(3):
                advect = advect + centres[d] * 0.5 * (upper[d] - lower[d])
                spread = spread + nu_up[d] * (upper[d] - center) - nu_low[d] * (center - lower[d])
            impulse = jnp.zeros_like(center)
            for s in range(slots):
                impulse = impulse + jnp.where(planes[s] == x, sent[s, c], 0.0)
            out[c, x] = center + 0.25 * (spread - advect) + impulse
        return carry

    lax.fori_loop(0, u.shape[1], plane, 0)


def vmem_call(kernel, out_shape, count, smem=0):
    specs = [pl.BlockSpec(memory_space=pltpu.SMEM)] * smem
    specs += [pl.BlockSpec(memory_space=pltpu.VMEM)] * (count - smem)
    return pl.pallas_call(
        kernel,
        out_shape=out_shape,
        in_specs=specs,
        out_specs=pl.BlockSpec(memory_space=pltpu.VMEM),
        interpret=INTERPRET,
    )


def stencil(velocity, planes, sent):
    nx = velocity.shape[1]
    u_faces = faces(velocity, 1)
    u_cols = jnp.concatenate(u_faces[4:], axis=0)
    nu = vmem_call(
        viscosity_kernel, jax.ShapeDtypeStruct(velocity.shape[1:], jnp.float32), 6
    )(velocity, *u_faces[:4], u_cols.reshape(-1, nx))
    nu_faces = faces(nu, 0)
    cols = jnp.concatenate([u_cols] + [f[None] for f in nu_faces[4:]], axis=0)
    return vmem_call(
        advance_kernel, jax.ShapeDtypeStruct(velocity.shape, jnp.float32), 13, smem=1
    )(planes, velocity, *u_faces[:4], nu, *nu_faces[:4], cols.reshape(-1, nx), sent)


def body(velocity, tile_turbine, tile_plane, tile_weight, chord):
    cx = velocity.shape[1]
    vertical_coord = velocity.shape[2]
    spanwise_coord = velocity.shape[3]
    tile_count = tile_turbine.shape[3]
    actuator_count = tile_weight.shape[4]
    nturb = chord.shape[0]
    turbine_list = tile_turbine.reshape(tile_count)
    rotor_planes = tile_plane.reshape(tile_count)
    spread_weights = tile_weight.reshape(
        tile_count, actuator_count, vertical_coord * spanwise_coord
    )
    flat = velocity.reshape(3, cx, vertical_coord * spanwise_coord)
    picks = (rotor_planes[:, None] == jnp.arange(cx, dtype=jnp.int32)[None, :]).astype(jnp.float32)
    tiles = jnp.einsum("sx,cxq->scq", picks, flat, precision=lax.Precision.HIGHEST).astype(
        jnp.bfloat16
    )
    block_local = jnp.einsum(
        "spq,scq->scp", spread_weights, tiles, preferred_element_type=jnp.float32
    )
    owning_block = (turbine_list[:, None] == jnp.arange(nturb, dtype=jnp.int32)[None, :]).astype(
        jnp.float32
    )
    partial_sample = jnp.einsum(
        "yr,yw->rw",
        owning_block,
        block_local.reshape(tile_count, -1),
        precision=lax.Precision.HIGHEST,
    )
    rows = lax.axis_size("gx")
    per_row = nturb // rows
    received = lax.all_to_all(
        partial_sample.reshape(rows, per_row, -1), "gx", split_axis=0, concat_axis=0, tiled=True
    )
    owned = jnp.sum(received, axis=0)
    for axis in ("gy", "gz"):
        count = lax.axis_size(axis)
        step = 1
        while step < count:
            pairs = [(i, i ^ step) for i in range(count)]
            owned = owned + lax.ppermute(owned, axis, pairs)
            step *= 2
    owned_coef = lax.dynamic_slice_in_dim(chord, lax.axis_index("gx") * per_row, per_row, 0)
    owned_force = actuate(owned, owned_coef)
    forces = lax.all_to_all(
        jnp.broadcast_to(owned_force[None], (rows,) + owned_force.shape),
        "gx", split_axis=0, concat_axis=0, tiled=True,
    ).reshape(nturb, -1)
    tile_force = jnp.dot(owning_block, forces, precision=lax.Precision.HIGHEST).astype(jnp.bfloat16)
    forces_sent = jnp.einsum(
        "axz,ahx->ahz",
        spread_weights,
        tile_force.reshape(tile_count, 3, actuator_count),
        preferred_element_type=jnp.float32,
    ).reshape(tile_count, 3, vertical_coord, spanwise_coord)
    predicted = stencil(velocity[:, :, :, :], rotor_planes, forces_sent)
    return (predicted, forces)


def solution(mesh):
    placed = (
        P(None, "gx", "gz", "gy"),
        P("gx", "gz", "gy", None),
        P("gx", "gz", "gy", None),
        P("gx", "gz", "gy", None, None, None),
        P(),
    )
    return jax.shard_map(
        body,
        mesh=mesh,
        in_specs=placed,
        out_specs=(P(None, "gx", "gz", "gy"), P()),
        check_vma=False,
    )
```

```python
import jax
import jax.numpy as jnp
from jax import lax
from jax.experimental import pallas as pl
from jax.experimental.pallas import tpu as pltpu
from jax.sharding import PartitionSpec as P

INTERPRET = False


def actuate(velocity_probe, coef):
    rows = velocity_probe.shape[0]
    parts = velocity_probe.reshape(rows, 3, -1)
    magnitude = jnp.sqrt(jnp.sum(parts * parts, axis=1) + 1e-06)
    return (-2.0 * coef[:, None, :] * magnitude[:, None, :] * parts).reshape(rows, -1)


def faces(block, lead):
    ny = block.shape[-1]
    ends = (lax.broadcasted_iota(jnp.int32, (2, ny), 1) == jnp.array([[0], [ny - 1]])).astype(jnp.float32)
    letters = "cxzy"[1 - lead :]
    columns = jnp.einsum(
        letters + ",ky->k" + letters[:-3] + "zx", block, ends, precision=lax.Precision.HIGHEST
    )
    out = []
    for axis, dim in (("gx", lead), ("gz", lead + 1), ("gy", None)):
        count = lax.axis_size(axis)
        forward = [(i, i + 1) for i in range(count - 1)]
        backward = [(target, source) for source, target in forward]
        if dim is None:
            first, last = columns[0], columns[1]
        else:
            size = block.shape[dim]
            first = lax.index_in_dim(block, 0, dim, keepdims=False)
            last = lax.index_in_dim(block, size - 1, dim, keepdims=False)
        out += [lax.ppermute(last, axis, forward), lax.ppermute(first, axis, backward)]
    return out


def neighbours(ref, xlo, xhi, zlo, zhi, ylo, yhi, lead, x, centre):
    nx = ref.shape[-3]
    nz, ny = centre.shape
    sub = lax.broadcasted_iota(jnp.int32, (nz, ny), 0)
    lane = lax.broadcasted_iota(jnp.int32, (nz, ny), 1)
    column = lax.broadcasted_iota(jnp.int32, (nz, nx), 1)
    prev = ref[lead + (jnp.maximum(x - 1, 0),)]
    nxt = ref[lead + (jnp.minimum(x + 1, nx - 1),)]
    xm = jnp.where(x == 0, xlo[lead], prev)
    xp = jnp.where(x == nx - 1, xhi[lead], nxt)
    zl = zlo[lead + (pl.ds(x, 1), slice(None))]
    zh = zhi[lead + (pl.ds(x, 1), slice(None))]
    zm = jnp.where(sub == 0, zl, pltpu.roll(centre, 1, 0))
    zp = jnp.where(sub == nz - 1, zh, pltpu.roll(centre, nz - 1, 0))
    yl = jnp.sum(jnp.where(column == x, ylo[lead], 0.0), axis=1, keepdims=True)
    yh = jnp.sum(jnp.where(column == x, yhi[lead], 0.0), axis=1, keepdims=True)
    ym = jnp.where(lane == 0, yl, pltpu.roll(centre, 1, 1))
    yp = jnp.where(lane == ny - 1, yh, pltpu.roll(centre, ny - 1, 1))
    return xm, xp, ym, yp, zm, zp


def viscosity_kernel(u, xlo, xhi, zlo, zhi, ylo, yhi, nu):
    def plane(x, carry):
        grads = []
        for c in range(3):
            xm, xp, ym, yp, zm, zp = neighbours(u, xlo, xhi, zlo, zhi, ylo, yhi, (c,), x, u[c, x])
            grads.append([0.5 * (xp - xm), 0.5 * (yp - ym), 0.5 * (zp - zm)])
        total = jnp.zeros_like(grads[0][0])
        for c in range(3):
            for d in range(3):
                strain = 0.5 * (grads[c][d] + grads[d][c])
                total = total + strain * strain
        nu[x] = 0.05 + 1.0 * jnp.sqrt(2.0 * total + 1e-06)
        return carry

    lax.fori_loop(0, u.shape[1], plane, 0)


def advance_kernel(planes, u, xlo, xhi, zlo, zhi, ylo, yhi, nu, nxlo, nxhi, nzlo, nzhi, nylo, nyhi, sent, out):
    slots = sent.shape[0]

    def plane(x, carry):
        here = nu[x]
        nxm, nxp, nym, nyp, nzm, nzp = neighbours(nu, nxlo, nxhi, nzlo, nzhi, nylo, nyhi, (), x, here)
        nu_up = [0.5 * (here + nxp), 0.5 * (here + nyp), 0.5 * (here + nzp)]
        nu_low = [0.5 * (here + nxm), 0.5 * (here + nym), 0.5 * (here + nzm)]
        centres = [u[c, x] for c in range(3)]
        for c in range(3):
            center = centres[c]
            xm, xp, ym, yp, zm, zp = neighbours(u, xlo, xhi, zlo, zhi, ylo, yhi, (c,), x, center)
            upper = (xp, yp, zp)
            lower = (xm, ym, zm)
            advect = jnp.zeros_like(center)
            spread = jnp.zeros_like(center)
            for d in range(3):
                advect = advect + centres[d] * 0.5 * (upper[d] - lower[d])
                spread = spread + nu_up[d] * (upper[d] - center) - nu_low[d] * (center - lower[d])
            impulse = jnp.zeros_like(center)
            for s in range(slots):
                impulse = impulse + jnp.where(planes[s] == x, sent[s, c], 0.0)
            out[c, x] = center + 0.25 * (spread - advect) + impulse
        return carry

    lax.fori_loop(0, u.shape[1], plane, 0)


def vmem_call(kernel, out_shape, count, smem=0):
    specs = [pl.BlockSpec(memory_space=pltpu.SMEM)] * smem
    specs += [pl.BlockSpec(memory_space=pltpu.VMEM)] * (count - smem)
    return pl.pallas_call(
        kernel,
        out_shape=out_shape,
        in_specs=specs,
        out_specs=pl.BlockSpec(memory_space=pltpu.VMEM),
        interpret=INTERPRET,
    )


def stencil(velocity, planes, sent):
    u_faces = faces(velocity, 1)
    nu = vmem_call(
        viscosity_kernel, jax.ShapeDtypeStruct(velocity.shape[1:], jnp.float32), 7
    )(velocity, *u_faces)
    nu_faces = faces(nu, 0)
    return vmem_call(
        advance_kernel, jax.ShapeDtypeStruct(velocity.shape, jnp.float32), 16, smem=1
    )(planes, velocity, *u_faces, nu, *nu_faces, sent)


def body(velocity, tile_turbine, tile_plane, tile_weight, chord):
    cx = velocity.shape[1]
    vertical_coord = velocity.shape[2]
    spanwise_coord = velocity.shape[3]
    tile_count = tile_turbine.shape[3]
    actuator_count = tile_weight.shape[4]
    nturb = chord.shape[0]
    turbine_list = tile_turbine.reshape(tile_count)
    rotor_planes = tile_plane.reshape(tile_count)
    spread_weights = tile_weight.reshape(
        tile_count, actuator_count, vertical_coord * spanwise_coord
    )
    tiles = jnp.stack(
        [lax.dynamic_index_in_dim(velocity, rotor_planes[s], 1, keepdims=False) for s in range(tile_count)]
    ).reshape(tile_count, 3, vertical_coord * spanwise_coord).astype(jnp.bfloat16)
    block_local = jnp.einsum(
        "spq,scq->scp", spread_weights, tiles, preferred_element_type=jnp.float32
    )
    owning_block = (turbine_list[:, None] == jnp.arange(nturb, dtype=jnp.int32)[None, :]).astype(
        jnp.float32
    )
    partial_sample = jnp.einsum(
        "yr,yw->rw",
        owning_block,
        block_local.reshape(tile_count, -1),
        precision=lax.Precision.HIGHEST,
    )
    rows = lax.axis_size("gx")
    per_row = nturb // rows
    received = lax.all_to_all(
        partial_sample.reshape(rows, per_row, -1), "gx", split_axis=0, concat_axis=0, tiled=True
    )
    owned = jnp.sum(received, axis=0)
    for axis in ("gy", "gz"):
        count = lax.axis_size(axis)
        step = 1
        while step < count:
            pairs = [(i, i ^ step) for i in range(count)]
            owned = owned + lax.ppermute(owned, axis, pairs)
            step *= 2
    owned_coef = lax.dynamic_slice_in_dim(chord, lax.axis_index("gx") * per_row, per_row, 0)
    owned_force = actuate(owned, owned_coef)
    forces = lax.all_to_all(
        jnp.broadcast_to(owned_force[None], (rows,) + owned_force.shape),
        "gx", split_axis=0, concat_axis=0, tiled=True,
    ).reshape(nturb, -1)
    tile_force = jnp.dot(owning_block, forces, precision=lax.Precision.HIGHEST).astype(jnp.bfloat16)
    forces_sent = jnp.einsum(
        "axz,ahx->ahz",
        spread_weights,
        tile_force.reshape(tile_count, 3, actuator_count),
        preferred_element_type=jnp.float32,
    ).reshape(tile_count, 3, vertical_coord, spanwise_coord)
    predicted = stencil(velocity[:, :, :, :], rotor_planes, forces_sent)
    return (predicted, forces)


def solution(mesh):
    placed = (
        P(None, "gx", "gz", "gy"),
        P("gx", "gz", "gy", None),
        P("gx", "gz", "gy", None),
        P("gx", "gz", "gy", None, None, None),
        P(),
    )
    return jax.shard_map(
        body,
        mesh=mesh,
        in_specs=placed,
        out_specs=(P(None, "gx", "gz", "gy"), P()),
        check_vma=False,
    )
```

```python
import jax
import jax.numpy as jnp
from jax import lax
from jax.experimental import pallas as pl
from jax.experimental.pallas import tpu as pltpu
from jax.sharding import PartitionSpec as P

INTERPRET = False


def actuate(velocity_probe, coef):
    rows = velocity_probe.shape[0]
    parts = velocity_probe.reshape(rows, 3, -1)
    magnitude = jnp.sqrt(jnp.sum(parts * parts, axis=1) + 1e-06)
    return (-2.0 * coef[:, None, :] * magnitude[:, None, :] * parts).reshape(rows, -1)


def faces(block, lead):
    ny = block.shape[-1]
    ends = (lax.broadcasted_iota(jnp.int32, (2, ny), 1) == jnp.array([[0], [ny - 1]])).astype(jnp.float32)
    letters = "cxzy"[1 - lead :]
    columns = jnp.einsum(
        letters + ",ky->k" + letters[:-3] + "zx", block, ends, precision=lax.Precision.HIGHEST
    )
    out = []
    for axis, dim in (("gx", lead), ("gz", lead + 1), ("gy", None)):
        count = lax.axis_size(axis)
        forward = [(i, i + 1) for i in range(count - 1)]
        backward = [(target, source) for source, target in forward]
        if dim is None:
            first, last = columns[0], columns[1]
        else:
            size = block.shape[dim]
            first = lax.index_in_dim(block, 0, dim, keepdims=False)
            last = lax.index_in_dim(block, size - 1, dim, keepdims=False)
        out += [lax.ppermute(last, axis, forward), lax.ppermute(first, axis, backward)]
    return out


def neighbours(ref, xlo, xhi, zlo, zhi, ylo, yhi, lead, x, centre):
    nx = ref.shape[-3]
    nz, ny = centre.shape
    sub = lax.broadcasted_iota(jnp.int32, (nz, ny), 0)
    lane = lax.broadcasted_iota(jnp.int32, (nz, ny), 1)
    column = lax.broadcasted_iota(jnp.int32, (nz, nx), 1)
    prev = ref[lead + (jnp.maximum(x - 1, 0),)]
    nxt = ref[lead + (jnp.minimum(x + 1, nx - 1),)]
    xm = jnp.where(x == 0, xlo[lead], prev)
    xp = jnp.where(x == nx - 1, xhi[lead], nxt)
    zl = zlo[lead + (pl.ds(x, 1), slice(None))]
    zh = zhi[lead + (pl.ds(x, 1), slice(None))]
    zm = jnp.where(sub == 0, zl, pltpu.roll(centre, 1, 0))
    zp = jnp.where(sub == nz - 1, zh, pltpu.roll(centre, nz - 1, 0))
    yl = jnp.sum(jnp.where(column == x, ylo[lead], 0.0), axis=1, keepdims=True)
    yh = jnp.sum(jnp.where(column == x, yhi[lead], 0.0), axis=1, keepdims=True)
    ym = jnp.where(lane == 0, yl, pltpu.roll(centre, 1, 1))
    yp = jnp.where(lane == ny - 1, yh, pltpu.roll(centre, ny - 1, 1))
    return xm, xp, ym, yp, zm, zp


def viscosity_kernel(u, xlo, xhi, zlo, zhi, ylo, yhi, nu):
    def plane(x, carry):
        grads = []
        for c in range(3):
            xm, xp, ym, yp, zm, zp = neighbours(u, xlo, xhi, zlo, zhi, ylo, yhi, (c,), x, u[c, x])
            grads.append([0.5 * (xp - xm), 0.5 * (yp - ym), 0.5 * (zp - zm)])
        total = jnp.zeros_like(grads[0][0])
        for c in range(3):
            for d in range(3):
                strain = 0.5 * (grads[c][d] + grads[d][c])
                total = total + strain * strain
        nu[x] = 0.05 + 1.0 * jnp.sqrt(2.0 * total + 1e-06)
        return carry

    lax.fori_loop(0, u.shape[1], plane, 0, unroll=2)


def advance_kernel(planes, u, xlo, xhi, zlo, zhi, ylo, yhi, nu, nxlo, nxhi, nzlo, nzhi, nylo, nyhi, sent, out):
    slots = sent.shape[0]

    def plane(x, carry):
        here = nu[x]
        nxm, nxp, nym, nyp, nzm, nzp = neighbours(nu, nxlo, nxhi, nzlo, nzhi, nylo, nyhi, (), x, here)
        nu_up = [0.5 * (here + nxp), 0.5 * (here + nyp), 0.5 * (here + nzp)]
        nu_low = [0.5 * (here + nxm), 0.5 * (here + nym), 0.5 * (here + nzm)]
        centres = [u[c, x] for c in range(3)]
        for c in range(3):
            center = centres[c]
            xm, xp, ym, yp, zm, zp = neighbours(u, xlo, xhi, zlo, zhi, ylo, yhi, (c,), x, center)
            upper = (xp, yp, zp)
            lower = (xm, ym, zm)
            advect = jnp.zeros_like(center)
            spread = jnp.zeros_like(center)
            for d in range(3):
                advect = advect + centres[d] * 0.5 * (upper[d] - lower[d])
                spread = spread + nu_up[d] * (upper[d] - center) - nu_low[d] * (center - lower[d])
            impulse = jnp.zeros_like(center)
            for s in range(slots):
                impulse = impulse + jnp.where(planes[s] == x, sent[s, c], 0.0)
            out[c, x] = center + 0.25 * (spread - advect) + impulse
        return carry

    lax.fori_loop(0, u.shape[1], plane, 0, unroll=2)


def vmem_call(kernel, out_shape, count, smem=0):
    specs = [pl.BlockSpec(memory_space=pltpu.SMEM)] * smem
    specs += [pl.BlockSpec(memory_space=pltpu.VMEM)] * (count - smem)
    return pl.pallas_call(
        kernel,
        out_shape=out_shape,
        in_specs=specs,
        out_specs=pl.BlockSpec(memory_space=pltpu.VMEM),
        interpret=INTERPRET,
    )


def stencil(velocity, planes, sent):
    u_faces = faces(velocity, 1)
    nu = vmem_call(
        viscosity_kernel, jax.ShapeDtypeStruct(velocity.shape[1:], jnp.float32), 7
    )(velocity, *u_faces)
    nu_faces = faces(nu, 0)
    return vmem_call(
        advance_kernel, jax.ShapeDtypeStruct(velocity.shape, jnp.float32), 16, smem=1
    )(planes, velocity, *u_faces, nu, *nu_faces, sent)


def body(velocity, tile_turbine, tile_plane, tile_weight, chord):
    cx = velocity.shape[1]
    vertical_coord = velocity.shape[2]
    spanwise_coord = velocity.shape[3]
    tile_count = tile_turbine.shape[3]
    actuator_count = tile_weight.shape[4]
    nturb = chord.shape[0]
    turbine_list = tile_turbine.reshape(tile_count)
    rotor_planes = tile_plane.reshape(tile_count)
    spread_weights = tile_weight.reshape(
        tile_count, actuator_count, vertical_coord * spanwise_coord
    )
    tiles = jnp.stack(
        [lax.dynamic_index_in_dim(velocity, rotor_planes[s], 1, keepdims=False) for s in range(tile_count)]
    ).reshape(tile_count, 3, vertical_coord * spanwise_coord).astype(jnp.bfloat16)
    block_local = jnp.einsum(
        "spq,scq->scp", spread_weights, tiles, preferred_element_type=jnp.float32
    )
    owning_block = (turbine_list[:, None] == jnp.arange(nturb, dtype=jnp.int32)[None, :]).astype(
        jnp.float32
    )
    partial_sample = jnp.einsum(
        "yr,yw->rw",
        owning_block,
        block_local.reshape(tile_count, -1),
        precision=lax.Precision.HIGHEST,
    )
    rows = lax.axis_size("gx")
    per_row = nturb // rows
    received = lax.all_to_all(
        partial_sample.reshape(rows, per_row, -1), "gx", split_axis=0, concat_axis=0, tiled=True
    )
    owned = jnp.sum(received, axis=0)
    for axis in ("gy", "gz"):
        count = lax.axis_size(axis)
        step = 1
        while step < count:
            pairs = [(i, i ^ step) for i in range(count)]
            owned = owned + lax.ppermute(owned, axis, pairs)
            step *= 2
    owned_coef = lax.dynamic_slice_in_dim(chord, lax.axis_index("gx") * per_row, per_row, 0)
    owned_force = actuate(owned, owned_coef)
    forces = lax.all_to_all(
        jnp.broadcast_to(owned_force[None], (rows,) + owned_force.shape),
        "gx", split_axis=0, concat_axis=0, tiled=True,
    ).reshape(nturb, -1)
    tile_force = jnp.dot(owning_block, forces, precision=lax.Precision.HIGHEST).astype(jnp.bfloat16)
    forces_sent = jnp.einsum(
        "axz,ahx->ahz",
        spread_weights,
        tile_force.reshape(tile_count, 3, actuator_count),
        preferred_element_type=jnp.float32,
    ).reshape(tile_count, 3, vertical_coord, spanwise_coord)
    predicted = stencil(velocity[:, :, :, :], rotor_planes, forces_sent)
    return (predicted, forces)


def solution(mesh):
    placed = (
        P(None, "gx", "gz", "gy"),
        P("gx", "gz", "gy", None),
        P("gx", "gz", "gy", None),
        P("gx", "gz", "gy", None, None, None),
        P(),
    )
    return jax.shard_map(
        body,
        mesh=mesh,
        in_specs=placed,
        out_specs=(P(None, "gx", "gz", "gy"), P()),
        check_vma=False,
    )
```

```python
import jax
import jax.numpy as jnp
from jax import lax
from jax.experimental import pallas as pl
from jax.experimental.pallas import tpu as pltpu
from jax.sharding import PartitionSpec as P

INTERPRET = False


def actuate(velocity_probe, coef):
    rows = velocity_probe.shape[0]
    parts = velocity_probe.reshape(rows, 3, -1)
    magnitude = jnp.sqrt(jnp.sum(parts * parts, axis=1) + 1e-06)
    return (-2.0 * coef[:, None, :] * magnitude[:, None, :] * parts).reshape(rows, -1)


def faces(block, lead):
    ny = block.shape[-1]
    ends = (lax.broadcasted_iota(jnp.int32, (2, ny), 1) == jnp.array([[0], [ny - 1]])).astype(jnp.float32)
    letters = "cxzy"[1 - lead :]
    columns = jnp.einsum(
        letters + ",ky->k" + letters[:-3] + "zx", block, ends, precision=lax.Precision.HIGHEST
    )
    out = []
    for axis, dim in (("gx", lead), ("gz", lead + 1), ("gy", None)):
        count = lax.axis_size(axis)
        forward = [(i, i + 1) for i in range(count - 1)]
        backward = [(target, source) for source, target in forward]
        if dim is None:
            first, last = columns[0], columns[1]
        else:
            size = block.shape[dim]
            first = lax.index_in_dim(block, 0, dim, keepdims=False)
            last = lax.index_in_dim(block, size - 1, dim, keepdims=False)
        out += [lax.ppermute(last, axis, forward), lax.ppermute(first, axis, backward)]
    return out


def neighbours(ref, xlo, xhi, zlo, zhi, ylo, yhi, lead, x, centre):
    nx = ref.shape[-3]
    nz, ny = centre.shape
    sub = lax.broadcasted_iota(jnp.int32, (nz, ny), 0)
    lane = lax.broadcasted_iota(jnp.int32, (nz, ny), 1)
    column = lax.broadcasted_iota(jnp.int32, (nz, nx), 1)
    prev = ref[lead + (jnp.maximum(x - 1, 0),)]
    nxt = ref[lead + (jnp.minimum(x + 1, nx - 1),)]
    xm = jnp.where(x == 0, xlo[lead], prev)
    xp = jnp.where(x == nx - 1, xhi[lead], nxt)
    zl = zlo[lead + (pl.ds(x, 1), slice(None))]
    zh = zhi[lead + (pl.ds(x, 1), slice(None))]
    zm = jnp.where(sub == 0, zl, pltpu.roll(centre, 1, 0))
    zp = jnp.where(sub == nz - 1, zh, pltpu.roll(centre, nz - 1, 0))
    yl = jnp.sum(jnp.where(column == x, ylo[lead], 0.0), axis=1, keepdims=True)
    yh = jnp.sum(jnp.where(column == x, yhi[lead], 0.0), axis=1, keepdims=True)
    ym = jnp.where(lane == 0, yl, pltpu.roll(centre, 1, 1))
    yp = jnp.where(lane == ny - 1, yh, pltpu.roll(centre, ny - 1, 1))
    return xm, xp, ym, yp, zm, zp


def viscosity_kernel(u, xlo, xhi, zlo, zhi, ylo, yhi, nu):
    def plane(x, carry):
        grads = []
        for c in range(3):
            xm, xp, ym, yp, zm, zp = neighbours(u, xlo, xhi, zlo, zhi, ylo, yhi, (c,), x, u[c, x])
            grads.append([0.5 * (xp - xm), 0.5 * (yp - ym), 0.5 * (zp - zm)])
        total = jnp.zeros_like(grads[0][0])
        for c in range(3):
            for d in range(3):
                strain = 0.5 * (grads[c][d] + grads[d][c])
                total = total + strain * strain
        nu[x] = 0.05 + 1.0 * jnp.sqrt(2.0 * total + 1e-06)
        return carry

    lax.fori_loop(0, u.shape[1], plane, 0, unroll=4)


def advance_kernel(planes, u, xlo, xhi, zlo, zhi, ylo, yhi, nu, nxlo, nxhi, nzlo, nzhi, nylo, nyhi, sent, out):
    slots = sent.shape[0]

    def plane(x, carry):
        here = nu[x]
        nxm, nxp, nym, nyp, nzm, nzp = neighbours(nu, nxlo, nxhi, nzlo, nzhi, nylo, nyhi, (), x, here)
        nu_up = [0.5 * (here + nxp), 0.5 * (here + nyp), 0.5 * (here + nzp)]
        nu_low = [0.5 * (here + nxm), 0.5 * (here + nym), 0.5 * (here + nzm)]
        centres = [u[c, x] for c in range(3)]
        for c in range(3):
            center = centres[c]
            xm, xp, ym, yp, zm, zp = neighbours(u, xlo, xhi, zlo, zhi, ylo, yhi, (c,), x, center)
            upper = (xp, yp, zp)
            lower = (xm, ym, zm)
            advect = jnp.zeros_like(center)
            spread = jnp.zeros_like(center)
            for d in range(3):
                advect = advect + centres[d] * 0.5 * (upper[d] - lower[d])
                spread = spread + nu_up[d] * (upper[d] - center) - nu_low[d] * (center - lower[d])
            impulse = jnp.zeros_like(center)
            for s in range(slots):
                impulse = impulse + jnp.where(planes[s] == x, sent[s, c], 0.0)
            out[c, x] = center + 0.25 * (spread - advect) + impulse
        return carry

    lax.fori_loop(0, u.shape[1], plane, 0, unroll=4)


def vmem_call(kernel, out_shape, count, smem=0):
    specs = [pl.BlockSpec(memory_space=pltpu.SMEM)] * smem
    specs += [pl.BlockSpec(memory_space=pltpu.VMEM)] * (count - smem)
    return pl.pallas_call(
        kernel,
        out_shape=out_shape,
        in_specs=specs,
        out_specs=pl.BlockSpec(memory_space=pltpu.VMEM),
        interpret=INTERPRET,
    )


def stencil(velocity, planes, sent):
    u_faces = faces(velocity, 1)
    nu = vmem_call(
        viscosity_kernel, jax.ShapeDtypeStruct(velocity.shape[1:], jnp.float32), 7
    )(velocity, *u_faces)
    nu_faces = faces(nu, 0)
    return vmem_call(
        advance_kernel, jax.ShapeDtypeStruct(velocity.shape, jnp.float32), 16, smem=1
    )(planes, velocity, *u_faces, nu, *nu_faces, sent)


def body(velocity, tile_turbine, tile_plane, tile_weight, chord):
    cx = velocity.shape[1]
    vertical_coord = velocity.shape[2]
    spanwise_coord = velocity.shape[3]
    tile_count = tile_turbine.shape[3]
    actuator_count = tile_weight.shape[4]
    nturb = chord.shape[0]
    turbine_list = tile_turbine.reshape(tile_count)
    rotor_planes = tile_plane.reshape(tile_count)
    spread_weights = tile_weight.reshape(
        tile_count, actuator_count, vertical_coord * spanwise_coord
    )
    tiles = jnp.stack(
        [lax.dynamic_index_in_dim(velocity, rotor_planes[s], 1, keepdims=False) for s in range(tile_count)]
    ).reshape(tile_count, 3, vertical_coord * spanwise_coord).astype(jnp.bfloat16)
    block_local = jnp.einsum(
        "spq,scq->scp", spread_weights, tiles, preferred_element_type=jnp.float32
    )
    owning_block = (turbine_list[:, None] == jnp.arange(nturb, dtype=jnp.int32)[None, :]).astype(
        jnp.float32
    )
    partial_sample = jnp.einsum(
        "yr,yw->rw",
        owning_block,
        block_local.reshape(tile_count, -1),
        precision=lax.Precision.HIGHEST,
    )
    rows = lax.axis_size("gx")
    per_row = nturb // rows
    received = lax.all_to_all(
        partial_sample.reshape(rows, per_row, -1), "gx", split_axis=0, concat_axis=0, tiled=True
    )
    owned = jnp.sum(received, axis=0)
    for axis in ("gy", "gz"):
        count = lax.axis_size(axis)
        step = 1
        while step < count:
            pairs = [(i, i ^ step) for i in range(count)]
            owned = owned + lax.ppermute(owned, axis, pairs)
            step *= 2
    owned_coef = lax.dynamic_slice_in_dim(chord, lax.axis_index("gx") * per_row, per_row, 0)
    owned_force = actuate(owned, owned_coef)
    forces = lax.all_to_all(
        jnp.broadcast_to(owned_force[None], (rows,) + owned_force.shape),
        "gx", split_axis=0, concat_axis=0, tiled=True,
    ).reshape(nturb, -1)
    tile_force = jnp.dot(owning_block, forces, precision=lax.Precision.HIGHEST).astype(jnp.bfloat16)
    forces_sent = jnp.einsum(
        "axz,ahx->ahz",
        spread_weights,
        tile_force.reshape(tile_count, 3, actuator_count),
        preferred_element_type=jnp.float32,
    ).reshape(tile_count, 3, vertical_coord, spanwise_coord)
    predicted = stencil(velocity[:, :, :, :], rotor_planes, forces_sent)
    return (predicted, forces)


def solution(mesh):
    placed = (
        P(None, "gx", "gz", "gy"),
        P("gx", "gz", "gy", None),
        P("gx", "gz", "gy", None),
        P("gx", "gz", "gy", None, None, None),
        P(),
    )
    return jax.shard_map(
        body,
        mesh=mesh,
        in_specs=placed,
        out_specs=(P(None, "gx", "gz", "gy"), P()),
        check_vma=False,
    )
```

```python
import jax
import jax.numpy as jnp
from jax import lax
from jax.experimental import pallas as pl
from jax.experimental.pallas import tpu as pltpu
from jax.sharding import PartitionSpec as P

INTERPRET = False


def actuate(velocity_probe, coef):
    rows = velocity_probe.shape[0]
    parts = velocity_probe.reshape(rows, 3, -1)
    magnitude = jnp.sqrt(jnp.sum(parts * parts, axis=1) + 1e-06)
    return (-2.0 * coef[:, None, :] * magnitude[:, None, :] * parts).reshape(rows, -1)


def faces(block, lead):
    ny = block.shape[-1]
    ends = (lax.broadcasted_iota(jnp.int32, (2, ny), 1) == jnp.array([[0], [ny - 1]])).astype(jnp.float32)
    letters = "cxzy"[1 - lead :]
    columns = jnp.einsum(
        letters + ",ky->k" + letters[:-3] + "zx", block, ends, precision=lax.Precision.HIGHEST
    )
    out = []
    for axis, dim in (("gx", lead), ("gz", lead + 1), ("gy", None)):
        count = lax.axis_size(axis)
        forward = [(i, i + 1) for i in range(count - 1)]
        backward = [(target, source) for source, target in forward]
        if dim is None:
            first, last = columns[0], columns[1]
        else:
            size = block.shape[dim]
            first = lax.index_in_dim(block, 0, dim, keepdims=False)
            last = lax.index_in_dim(block, size - 1, dim, keepdims=False)
        out += [lax.ppermute(last, axis, forward), lax.ppermute(first, axis, backward)]
    return out


def neighbours(ref, xlo, xhi, zlo, zhi, ylo, yhi, lead, x, centre):
    nx = ref.shape[-3]
    nz, ny = centre.shape
    sub = lax.broadcasted_iota(jnp.int32, (nz, ny), 0)
    lane = lax.broadcasted_iota(jnp.int32, (nz, ny), 1)
    column = lax.broadcasted_iota(jnp.int32, (nz, nx), 1)
    prev = ref[lead + (jnp.maximum(x - 1, 0),)]
    nxt = ref[lead + (jnp.minimum(x + 1, nx - 1),)]
    xm = jnp.where(x == 0, xlo[lead], prev)
    xp = jnp.where(x == nx - 1, xhi[lead], nxt)
    zl = zlo[lead + (pl.ds(x, 1), slice(None))]
    zh = zhi[lead + (pl.ds(x, 1), slice(None))]
    zm = jnp.where(sub == 0, zl, pltpu.roll(centre, 1, 0))
    zp = jnp.where(sub == nz - 1, zh, pltpu.roll(centre, nz - 1, 0))
    yl = jnp.sum(jnp.where(column == x, ylo[lead], 0.0), axis=1, keepdims=True)
    yh = jnp.sum(jnp.where(column == x, yhi[lead], 0.0), axis=1, keepdims=True)
    ym = jnp.where(lane == 0, yl, pltpu.roll(centre, 1, 1))
    yp = jnp.where(lane == ny - 1, yh, pltpu.roll(centre, ny - 1, 1))
    return xm, xp, ym, yp, zm, zp


def viscosity_kernel(u, xlo, xhi, zlo, zhi, ylo, yhi, nu):
    def plane(x, carry):
        grads = []
        for c in range(3):
            xm, xp, ym, yp, zm, zp = neighbours(u, xlo, xhi, zlo, zhi, ylo, yhi, (c,), x, u[c, x])
            grads.append([0.5 * (xp - xm), 0.5 * (yp - ym), 0.5 * (zp - zm)])
        total = jnp.zeros_like(grads[0][0])
        for c in range(3):
            for d in range(3):
                strain = 0.5 * (grads[c][d] + grads[d][c])
                total = total + strain * strain
        nu[x] = 0.05 + 1.0 * jnp.sqrt(2.0 * total + 1e-06)
        return carry

    lax.fori_loop(0, u.shape[1], plane, 0, unroll=8)


def advance_kernel(planes, u, xlo, xhi, zlo, zhi, ylo, yhi, nu, nxlo, nxhi, nzlo, nzhi, nylo, nyhi, sent, out):
    slots = sent.shape[0]

    def plane(x, carry):
        here = nu[x]
        nxm, nxp, nym, nyp, nzm, nzp = neighbours(nu, nxlo, nxhi, nzlo, nzhi, nylo, nyhi, (), x, here)
        nu_up = [0.5 * (here + nxp), 0.5 * (here + nyp), 0.5 * (here + nzp)]
        nu_low = [0.5 * (here + nxm), 0.5 * (here + nym), 0.5 * (here + nzm)]
        centres = [u[c, x] for c in range(3)]
        for c in range(3):
            center = centres[c]
            xm, xp, ym, yp, zm, zp = neighbours(u, xlo, xhi, zlo, zhi, ylo, yhi, (c,), x, center)
            upper = (xp, yp, zp)
            lower = (xm, ym, zm)
            advect = jnp.zeros_like(center)
            spread = jnp.zeros_like(center)
            for d in range(3):
                advect = advect + centres[d] * 0.5 * (upper[d] - lower[d])
                spread = spread + nu_up[d] * (upper[d] - center) - nu_low[d] * (center - lower[d])
            impulse = jnp.zeros_like(center)
            for s in range(slots):
                impulse = impulse + jnp.where(planes[s] == x, sent[s, c], 0.0)
            out[c, x] = center + 0.25 * (spread - advect) + impulse
        return carry

    lax.fori_loop(0, u.shape[1], plane, 0, unroll=8)


def vmem_call(kernel, out_shape, count, smem=0):
    specs = [pl.BlockSpec(memory_space=pltpu.SMEM)] * smem
    specs += [pl.BlockSpec(memory_space=pltpu.VMEM)] * (count - smem)
    return pl.pallas_call(
        kernel,
        out_shape=out_shape,
        in_specs=specs,
        out_specs=pl.BlockSpec(memory_space=pltpu.VMEM),
        interpret=INTERPRET,
    )


def stencil(velocity, planes, sent):
    u_faces = faces(velocity, 1)
    nu = vmem_call(
        viscosity_kernel, jax.ShapeDtypeStruct(velocity.shape[1:], jnp.float32), 7
    )(velocity, *u_faces)
    nu_faces = faces(nu, 0)
    return vmem_call(
        advance_kernel, jax.ShapeDtypeStruct(velocity.shape, jnp.float32), 16, smem=1
    )(planes, velocity, *u_faces, nu, *nu_faces, sent)


def body(velocity, tile_turbine, tile_plane, tile_weight, chord):
    cx = velocity.shape[1]
    vertical_coord = velocity.shape[2]
    spanwise_coord = velocity.shape[3]
    tile_count = tile_turbine.shape[3]
    actuator_count = tile_weight.shape[4]
    nturb = chord.shape[0]
    turbine_list = tile_turbine.reshape(tile_count)
    rotor_planes = tile_plane.reshape(tile_count)
    spread_weights = tile_weight.reshape(
        tile_count, actuator_count, vertical_coord * spanwise_coord
    )
    tiles = jnp.stack(
        [lax.dynamic_index_in_dim(velocity, rotor_planes[s], 1, keepdims=False) for s in range(tile_count)]
    ).reshape(tile_count, 3, vertical_coord * spanwise_coord).astype(jnp.bfloat16)
    block_local = jnp.einsum(
        "spq,scq->scp", spread_weights, tiles, preferred_element_type=jnp.float32
    )
    owning_block = (turbine_list[:, None] == jnp.arange(nturb, dtype=jnp.int32)[None, :]).astype(
        jnp.float32
    )
    partial_sample = jnp.einsum(
        "yr,yw->rw",
        owning_block,
        block_local.reshape(tile_count, -1),
        precision=lax.Precision.HIGHEST,
    )
    rows = lax.axis_size("gx")
    per_row = nturb // rows
    received = lax.all_to_all(
        partial_sample.reshape(rows, per_row, -1), "gx", split_axis=0, concat_axis=0, tiled=True
    )
    owned = jnp.sum(received, axis=0)
    for axis in ("gy", "gz"):
        count = lax.axis_size(axis)
        step = 1
        while step < count:
            pairs = [(i, i ^ step) for i in range(count)]
            owned = owned + lax.ppermute(owned, axis, pairs)
            step *= 2
    owned_coef = lax.dynamic_slice_in_dim(chord, lax.axis_index("gx") * per_row, per_row, 0)
    owned_force = actuate(owned, owned_coef)
    forces = lax.all_to_all(
        jnp.broadcast_to(owned_force[None], (rows,) + owned_force.shape),
        "gx", split_axis=0, concat_axis=0, tiled=True,
    ).reshape(nturb, -1)
    tile_force = jnp.dot(owning_block, forces, precision=lax.Precision.HIGHEST).astype(jnp.bfloat16)
    forces_sent = jnp.einsum(
        "axz,ahx->ahz",
        spread_weights,
        tile_force.reshape(tile_count, 3, actuator_count),
        preferred_element_type=jnp.float32,
    ).reshape(tile_count, 3, vertical_coord, spanwise_coord)
    predicted = stencil(velocity[:, :, :, :], rotor_planes, forces_sent)
    return (predicted, forces)


def solution(mesh):
    placed = (
        P(None, "gx", "gz", "gy"),
        P("gx", "gz", "gy", None),
        P("gx", "gz", "gy", None),
        P("gx", "gz", "gy", None, None, None),
        P(),
    )
    return jax.shard_map(
        body,
        mesh=mesh,
        in_specs=placed,
        out_specs=(P(None, "gx", "gz", "gy"), P()),
        check_vma=False,
    )
```

```python
import jax
import jax.numpy as jnp
from jax import lax
from jax.experimental import pallas as pl
from jax.experimental.pallas import tpu as pltpu
from jax.sharding import PartitionSpec as P

INTERPRET = False


def actuate(velocity_probe, coef):
    rows = velocity_probe.shape[0]
    parts = velocity_probe.reshape(rows, 3, -1)
    magnitude = jnp.sqrt(jnp.sum(parts * parts, axis=1) + 1e-06)
    return (-2.0 * coef[:, None, :] * magnitude[:, None, :] * parts).reshape(rows, -1)


def faces(block, lead):
    ny = block.shape[-1]
    lane = lax.broadcasted_iota(jnp.int32, block.shape, block.ndim - 1)
    columns = [
        jnp.swapaxes(jnp.sum(jnp.where(lane == y, block, 0.0), axis=-1), -1, -2) for y in (0, ny - 1)
    ]
    out = []
    for axis, dim in (("gx", lead), ("gz", lead + 1), ("gy", None)):
        count = lax.axis_size(axis)
        forward = [(i, i + 1) for i in range(count - 1)]
        backward = [(target, source) for source, target in forward]
        if dim is None:
            first, last = columns[0], columns[1]
        else:
            size = block.shape[dim]
            first = lax.index_in_dim(block, 0, dim, keepdims=False)
            last = lax.index_in_dim(block, size - 1, dim, keepdims=False)
        out += [lax.ppermute(last, axis, forward), lax.ppermute(first, axis, backward)]
    return out


def neighbours(ref, xlo, xhi, zlo, zhi, ylo, yhi, lead, x, centre):
    nx = ref.shape[-3]
    nz, ny = centre.shape
    sub = lax.broadcasted_iota(jnp.int32, (nz, ny), 0)
    lane = lax.broadcasted_iota(jnp.int32, (nz, ny), 1)
    column = lax.broadcasted_iota(jnp.int32, (nz, nx), 1)
    prev = ref[lead + (jnp.maximum(x - 1, 0),)]
    nxt = ref[lead + (jnp.minimum(x + 1, nx - 1),)]
    xm = jnp.where(x == 0, xlo[lead], prev)
    xp = jnp.where(x == nx - 1, xhi[lead], nxt)
    zl = zlo[lead + (pl.ds(x, 1), slice(None))]
    zh = zhi[lead + (pl.ds(x, 1), slice(None))]
    zm = jnp.where(sub == 0, zl, pltpu.roll(centre, 1, 0))
    zp = jnp.where(sub == nz - 1, zh, pltpu.roll(centre, nz - 1, 0))
    yl = jnp.sum(jnp.where(column == x, ylo[lead], 0.0), axis=1, keepdims=True)
    yh = jnp.sum(jnp.where(column == x, yhi[lead], 0.0), axis=1, keepdims=True)
    ym = jnp.where(lane == 0, yl, pltpu.roll(centre, 1, 1))
    yp = jnp.where(lane == ny - 1, yh, pltpu.roll(centre, ny - 1, 1))
    return xm, xp, ym, yp, zm, zp


def viscosity_kernel(u, xlo, xhi, zlo, zhi, ylo, yhi, nu):
    def plane(x, carry):
        grads = []
        for c in range(3):
            xm, xp, ym, yp, zm, zp = neighbours(u, xlo, xhi, zlo, zhi, ylo, yhi, (c,), x, u[c, x])
            grads.append([0.5 * (xp - xm), 0.5 * (yp - ym), 0.5 * (zp - zm)])
        total = jnp.zeros_like(grads[0][0])
        for c in range(3):
            for d in range(3):
                strain = 0.5 * (grads[c][d] + grads[d][c])
                total = total + strain * strain
        nu[x] = 0.05 + 1.0 * jnp.sqrt(2.0 * total + 1e-06)
        return carry

    lax.fori_loop(0, u.shape[1], plane, 0, unroll=8)


def advance_kernel(planes, u, xlo, xhi, zlo, zhi, ylo, yhi, nu, nxlo, nxhi, nzlo, nzhi, nylo, nyhi, sent, out):
    slots = sent.shape[0]

    def plane(x, carry):
        here = nu[x]
        nxm, nxp, nym, nyp, nzm, nzp = neighbours(nu, nxlo, nxhi, nzlo, nzhi, nylo, nyhi, (), x, here)
        nu_up = [0.5 * (here + nxp), 0.5 * (here + nyp), 0.5 * (here + nzp)]
        nu_low = [0.5 * (here + nxm), 0.5 * (here + nym), 0.5 * (here + nzm)]
        centres = [u[c, x] for c in range(3)]
        for c in range(3):
            center = centres[c]
            xm, xp, ym, yp, zm, zp = neighbours(u, xlo, xhi, zlo, zhi, ylo, yhi, (c,), x, center)
            upper = (xp, yp, zp)
            lower = (xm, ym, zm)
            advect = jnp.zeros_like(center)
            spread = jnp.zeros_like(center)
            for d in range(3):
                advect = advect + centres[d] * 0.5 * (upper[d] - lower[d])
                spread = spread + nu_up[d] * (upper[d] - center) - nu_low[d] * (center - lower[d])
            impulse = jnp.zeros_like(center)
            for s in range(slots):
                impulse = impulse + jnp.where(planes[s] == x, sent[s, c], 0.0)
            out[c, x] = center + 0.25 * (spread - advect) + impulse
        return carry

    lax.fori_loop(0, u.shape[1], plane, 0, unroll=8)


def vmem_call(kernel, out_shape, count, smem=0):
    specs = [pl.BlockSpec(memory_space=pltpu.SMEM)] * smem
    specs += [pl.BlockSpec(memory_space=pltpu.VMEM)] * (count - smem)
    return pl.pallas_call(
        kernel,
        out_shape=out_shape,
        in_specs=specs,
        out_specs=pl.BlockSpec(memory_space=pltpu.VMEM),
        interpret=INTERPRET,
    )


def stencil(velocity, planes, sent):
    u_faces = faces(velocity, 1)
    nu = vmem_call(
        viscosity_kernel, jax.ShapeDtypeStruct(velocity.shape[1:], jnp.float32), 7
    )(velocity, *u_faces)
    nu_faces = faces(nu, 0)
    return vmem_call(
        advance_kernel, jax.ShapeDtypeStruct(velocity.shape, jnp.float32), 16, smem=1
    )(planes, velocity, *u_faces, nu, *nu_faces, sent)


def body(velocity, tile_turbine, tile_plane, tile_weight, chord):
    cx = velocity.shape[1]
    vertical_coord = velocity.shape[2]
    spanwise_coord = velocity.shape[3]
    tile_count = tile_turbine.shape[3]
    actuator_count = tile_weight.shape[4]
    nturb = chord.shape[0]
    turbine_list = tile_turbine.reshape(tile_count)
    rotor_planes = tile_plane.reshape(tile_count)
    spread_weights = tile_weight.reshape(
        tile_count, actuator_count, vertical_coord * spanwise_coord
    )
    tiles = jnp.stack(
        [lax.dynamic_index_in_dim(velocity, rotor_planes[s], 1, keepdims=False) for s in range(tile_count)]
    ).reshape(tile_count, 3, vertical_coord * spanwise_coord).astype(jnp.bfloat16)
    block_local = jnp.einsum(
        "spq,scq->scp", spread_weights, tiles, preferred_element_type=jnp.float32
    )
    owning_block = (turbine_list[:, None] == jnp.arange(nturb, dtype=jnp.int32)[None, :]).astype(
        jnp.float32
    )
    partial_sample = jnp.einsum(
        "yr,yw->rw",
        owning_block,
        block_local.reshape(tile_count, -1),
        precision=lax.Precision.HIGHEST,
    )
    rows = lax.axis_size("gx")
    per_row = nturb // rows
    received = lax.all_to_all(
        partial_sample.reshape(rows, per_row, -1), "gx", split_axis=0, concat_axis=0, tiled=True
    )
    owned = jnp.sum(received, axis=0)
    for axis in ("gy", "gz"):
        count = lax.axis_size(axis)
        step = 1
        while step < count:
            pairs = [(i, i ^ step) for i in range(count)]
            owned = owned + lax.ppermute(owned, axis, pairs)
            step *= 2
    owned_coef = lax.dynamic_slice_in_dim(chord, lax.axis_index("gx") * per_row, per_row, 0)
    owned_force = actuate(owned, owned_coef)
    forces = lax.all_to_all(
        jnp.broadcast_to(owned_force[None], (rows,) + owned_force.shape),
        "gx", split_axis=0, concat_axis=0, tiled=True,
    ).reshape(nturb, -1)
    tile_force = jnp.dot(owning_block, forces, precision=lax.Precision.HIGHEST).astype(jnp.bfloat16)
    forces_sent = jnp.einsum(
        "axz,ahx->ahz",
        spread_weights,
        tile_force.reshape(tile_count, 3, actuator_count),
        preferred_element_type=jnp.float32,
    ).reshape(tile_count, 3, vertical_coord, spanwise_coord)
    predicted = stencil(velocity[:, :, :, :], rotor_planes, forces_sent)
    return (predicted, forces)


def solution(mesh):
    placed = (
        P(None, "gx", "gz", "gy"),
        P("gx", "gz", "gy", None),
        P("gx", "gz", "gy", None),
        P("gx", "gz", "gy", None, None, None),
        P(),
    )
    return jax.shard_map(
        body,
        mesh=mesh,
        in_specs=placed,
        out_specs=(P(None, "gx", "gz", "gy"), P()),
        check_vma=False,
    )
```

```python
import jax
import jax.numpy as jnp
from jax import lax
from jax.experimental import pallas as pl
from jax.experimental.pallas import tpu as pltpu
from jax.sharding import PartitionSpec as P

INTERPRET = False


def actuate(velocity_probe, coef):
    rows = velocity_probe.shape[0]
    parts = velocity_probe.reshape(rows, 3, -1)
    magnitude = jnp.sqrt(jnp.sum(parts * parts, axis=1) + 1e-06)
    return (-2.0 * coef[:, None, :] * magnitude[:, None, :] * parts).reshape(rows, -1)


def faces(block, lead):
    ny = block.shape[-1]
    lane = lax.broadcasted_iota(jnp.int32, block.shape, block.ndim - 1)
    columns = [
        jnp.swapaxes(jnp.sum(jnp.where(lane == y, block, 0.0), axis=-1), -1, -2) for y in (0, ny - 1)
    ]
    out = []
    for axis, dim in (("gx", lead), ("gz", lead + 1), ("gy", None)):
        count = lax.axis_size(axis)
        forward = [(i, i + 1) for i in range(count - 1)]
        backward = [(target, source) for source, target in forward]
        if dim is None:
            first, last = columns[0], columns[1]
        else:
            size = block.shape[dim]
            first = lax.index_in_dim(block, 0, dim, keepdims=False)
            last = lax.index_in_dim(block, size - 1, dim, keepdims=False)
        out += [lax.ppermute(last, axis, forward), lax.ppermute(first, axis, backward)]
    return out


def neighbours(ref, xlo, xhi, zlo, zhi, ylo, yhi, lead, x, centre):
    nx = ref.shape[-3]
    nz, ny = centre.shape
    sub = lax.broadcasted_iota(jnp.int32, (nz, ny), 0)
    lane = lax.broadcasted_iota(jnp.int32, (nz, ny), 1)
    column = lax.broadcasted_iota(jnp.int32, (nz, nx), 1)
    prev = ref[lead + (jnp.maximum(x - 1, 0),)]
    nxt = ref[lead + (jnp.minimum(x + 1, nx - 1),)]
    xm = jnp.where(x == 0, xlo[lead], prev)
    xp = jnp.where(x == nx - 1, xhi[lead], nxt)
    zl = zlo[lead + (pl.ds(x, 1), slice(None))]
    zh = zhi[lead + (pl.ds(x, 1), slice(None))]
    zm = jnp.where(sub == 0, zl, pltpu.roll(centre, 1, 0))
    zp = jnp.where(sub == nz - 1, zh, pltpu.roll(centre, nz - 1, 0))
    yl = jnp.sum(jnp.where(column == x, ylo[lead], 0.0), axis=1, keepdims=True)
    yh = jnp.sum(jnp.where(column == x, yhi[lead], 0.0), axis=1, keepdims=True)
    ym = jnp.where(lane == 0, yl, pltpu.roll(centre, 1, 1))
    yp = jnp.where(lane == ny - 1, yh, pltpu.roll(centre, ny - 1, 1))
    return xm, xp, ym, yp, zm, zp


def viscosity_kernel(u, xlo, xhi, zlo, zhi, ylo, yhi, nu):
    def plane(x, carry):
        grads = []
        for c in range(3):
            xm, xp, ym, yp, zm, zp = neighbours(u, xlo, xhi, zlo, zhi, ylo, yhi, (c,), x, u[c, x])
            grads.append([0.5 * (xp - xm), 0.5 * (yp - ym), 0.5 * (zp - zm)])
        total = jnp.zeros_like(grads[0][0])
        for c in range(3):
            for d in range(3):
                strain = 0.5 * (grads[c][d] + grads[d][c])
                total = total + strain * strain
        nu[x] = 0.05 + 1.0 * jnp.sqrt(2.0 * total + 1e-06)
        return carry

    lax.fori_loop(0, u.shape[1], plane, 0, unroll=8)


def advance_kernel(planes, u, xlo, xhi, zlo, zhi, ylo, yhi, nu, nxlo, nxhi, nzlo, nzhi, nylo, nyhi, sent, out):
    slots = sent.shape[0]

    def plane(x, carry):
        here = nu[x]
        nxm, nxp, nym, nyp, nzm, nzp = neighbours(nu, nxlo, nxhi, nzlo, nzhi, nylo, nyhi, (), x, here)
        nu_up = [0.5 * (here + nxp), 0.5 * (here + nyp), 0.5 * (here + nzp)]
        nu_low = [0.5 * (here + nxm), 0.5 * (here + nym), 0.5 * (here + nzm)]
        centres = [u[c, x] for c in range(3)]
        for c in range(3):
            center = centres[c]
            xm, xp, ym, yp, zm, zp = neighbours(u, xlo, xhi, zlo, zhi, ylo, yhi, (c,), x, center)
            upper = (xp, yp, zp)
            lower = (xm, ym, zm)
            advect = jnp.zeros_like(center)
            spread = jnp.zeros_like(center)
            for d in range(3):
                advect = advect + centres[d] * 0.5 * (upper[d] - lower[d])
                spread = spread + nu_up[d] * (upper[d] - center) - nu_low[d] * (center - lower[d])
            impulse = jnp.zeros_like(center)
            for s in range(slots):
                impulse = impulse + jnp.where(planes[s] == x, sent[s, c], 0.0)
            out[c, x] = center + 0.25 * (spread - advect) + impulse
        return carry

    lax.fori_loop(0, u.shape[1], plane, 0, unroll=8)


def vmem_call(kernel, out_shape, count, smem=0):
    specs = [pl.BlockSpec(memory_space=pltpu.SMEM)] * smem
    specs += [pl.BlockSpec(memory_space=pltpu.VMEM)] * (count - smem)
    return pl.pallas_call(
        kernel,
        out_shape=out_shape,
        in_specs=specs,
        out_specs=pl.BlockSpec(memory_space=pltpu.VMEM),
        interpret=INTERPRET,
    )


def stencil(velocity, planes, sent, u_faces):
    nu = vmem_call(
        viscosity_kernel, jax.ShapeDtypeStruct(velocity.shape[1:], jnp.float32), 7
    )(velocity, *u_faces)
    nu_faces = faces(nu, 0)
    return vmem_call(
        advance_kernel, jax.ShapeDtypeStruct(velocity.shape, jnp.float32), 16, smem=1
    )(planes, velocity, *u_faces, nu, *nu_faces, sent)


def body(velocity, tile_turbine, tile_plane, tile_weight, chord):
    cx = velocity.shape[1]
    vertical_coord = velocity.shape[2]
    spanwise_coord = velocity.shape[3]
    tile_count = tile_turbine.shape[3]
    actuator_count = tile_weight.shape[4]
    nturb = chord.shape[0]
    turbine_list = tile_turbine.reshape(tile_count)
    rotor_planes = tile_plane.reshape(tile_count)
    spread_weights = tile_weight.reshape(
        tile_count, actuator_count, vertical_coord * spanwise_coord
    )
    tiles = jnp.stack(
        [lax.dynamic_index_in_dim(velocity, rotor_planes[s], 1, keepdims=False) for s in range(tile_count)]
    ).reshape(tile_count, 3, vertical_coord * spanwise_coord).astype(jnp.bfloat16)
    block_local = jnp.einsum(
        "spq,scq->scp", spread_weights, tiles, preferred_element_type=jnp.float32
    )
    owning_block = (turbine_list[:, None] == jnp.arange(nturb, dtype=jnp.int32)[None, :]).astype(
        jnp.float32
    )
    partial_sample = jnp.einsum(
        "yr,yw->rw",
        owning_block,
        block_local.reshape(tile_count, -1),
        precision=lax.Precision.HIGHEST,
    )
    u_faces = faces(velocity, 1)
    partial_sample, u_faces = lax.optimization_barrier((partial_sample, u_faces))
    rows = lax.axis_size("gx")
    per_row = nturb // rows
    received = lax.all_to_all(
        partial_sample.reshape(rows, per_row, -1), "gx", split_axis=0, concat_axis=0, tiled=True
    )
    owned = jnp.sum(received, axis=0)
    for axis in ("gy", "gz"):
        count = lax.axis_size(axis)
        step = 1
        while step < count:
            pairs = [(i, i ^ step) for i in range(count)]
            owned = owned + lax.ppermute(owned, axis, pairs)
            step *= 2
    owned_coef = lax.dynamic_slice_in_dim(chord, lax.axis_index("gx") * per_row, per_row, 0)
    owned_force = actuate(owned, owned_coef)
    forces = lax.all_to_all(
        jnp.broadcast_to(owned_force[None], (rows,) + owned_force.shape),
        "gx", split_axis=0, concat_axis=0, tiled=True,
    ).reshape(nturb, -1)
    tile_force = jnp.dot(owning_block, forces, precision=lax.Precision.HIGHEST).astype(jnp.bfloat16)
    forces_sent = jnp.einsum(
        "axz,ahx->ahz",
        spread_weights,
        tile_force.reshape(tile_count, 3, actuator_count),
        preferred_element_type=jnp.float32,
    ).reshape(tile_count, 3, vertical_coord, spanwise_coord)
    predicted = stencil(velocity, rotor_planes, forces_sent, u_faces)
    return (predicted, forces)


def solution(mesh):
    placed = (
        P(None, "gx", "gz", "gy"),
        P("gx", "gz", "gy", None),
        P("gx", "gz", "gy", None),
        P("gx", "gz", "gy", None, None, None),
        P(),
    )
    return jax.shard_map(
        body,
        mesh=mesh,
        in_specs=placed,
        out_specs=(P(None, "gx", "gz", "gy"), P()),
        check_vma=False,
    )
```

```python
import jax
import jax.numpy as jnp
from jax import lax
from jax.experimental import pallas as pl
from jax.experimental.pallas import tpu as pltpu
from jax.sharding import PartitionSpec as P

INTERPRET = False


def actuate(velocity_probe, coef):
    rows = velocity_probe.shape[0]
    parts = velocity_probe.reshape(rows, 3, -1)
    magnitude = jnp.sqrt(jnp.sum(parts * parts, axis=1) + 1e-06)
    return (-2.0 * coef[:, None, :] * magnitude[:, None, :] * parts).reshape(rows, -1)


def faces(block, lead):
    ny = block.shape[-1]
    ends = (lax.broadcasted_iota(jnp.int32, (2, ny), 1) == jnp.array([[0], [ny - 1]])).astype(jnp.float32)
    letters = "cxzy"[1 - lead :]
    columns = jnp.einsum(
        letters + ",ky->k" + letters[:-3] + "zx", block, ends, precision=lax.Precision.HIGHEST
    )
    out = []
    for axis, dim in (("gx", lead), ("gz", lead + 1), ("gy", None)):
        count = lax.axis_size(axis)
        forward = [(i, i + 1) for i in range(count - 1)]
        backward = [(target, source) for source, target in forward]
        if dim is None:
            first, last = columns[0], columns[1]
        else:
            size = block.shape[dim]
            first = lax.index_in_dim(block, 0, dim, keepdims=False)
            last = lax.index_in_dim(block, size - 1, dim, keepdims=False)
        out += [lax.ppermute(last, axis, forward), lax.ppermute(first, axis, backward)]
    return out


def neighbours(ref, xlo, xhi, zlo, zhi, ylo, yhi, lead, x, centre):
    nx = ref.shape[-3]
    nz, ny = centre.shape
    sub = lax.broadcasted_iota(jnp.int32, (nz, ny), 0)
    lane = lax.broadcasted_iota(jnp.int32, (nz, ny), 1)
    column = lax.broadcasted_iota(jnp.int32, (nz, nx), 1)
    prev = ref[lead + (jnp.maximum(x - 1, 0),)]
    nxt = ref[lead + (jnp.minimum(x + 1, nx - 1),)]
    xm = jnp.where(x == 0, xlo[lead], prev)
    xp = jnp.where(x == nx - 1, xhi[lead], nxt)
    zl = zlo[lead + (pl.ds(x, 1), slice(None))]
    zh = zhi[lead + (pl.ds(x, 1), slice(None))]
    zm = jnp.where(sub == 0, zl, pltpu.roll(centre, 1, 0))
    zp = jnp.where(sub == nz - 1, zh, pltpu.roll(centre, nz - 1, 0))
    yl = jnp.sum(jnp.where(column == x, ylo[lead], 0.0), axis=1, keepdims=True)
    yh = jnp.sum(jnp.where(column == x, yhi[lead], 0.0), axis=1, keepdims=True)
    ym = jnp.where(lane == 0, yl, pltpu.roll(centre, 1, 1))
    yp = jnp.where(lane == ny - 1, yh, pltpu.roll(centre, ny - 1, 1))
    return xm, xp, ym, yp, zm, zp


def viscosity_kernel(u, xlo, xhi, zlo, zhi, ylo, yhi, nu):
    def plane(x, carry):
        grads = []
        for c in range(3):
            xm, xp, ym, yp, zm, zp = neighbours(u, xlo, xhi, zlo, zhi, ylo, yhi, (c,), x, u[c, x])
            grads.append([0.5 * (xp - xm), 0.5 * (yp - ym), 0.5 * (zp - zm)])
        total = jnp.zeros_like(grads[0][0])
        for c in range(3):
            for d in range(3):
                strain = 0.5 * (grads[c][d] + grads[d][c])
                total = total + strain * strain
        nu[x] = 0.05 + 1.0 * jnp.sqrt(2.0 * total + 1e-06)
        return carry

    lax.fori_loop(0, u.shape[1], plane, 0, unroll=8)


def advance_kernel(u, xlo, xhi, zlo, zhi, ylo, yhi, nu, nxlo, nxhi, nzlo, nzhi, nylo, nyhi, out):

    def plane(x, carry):
        here = nu[x]
        nxm, nxp, nym, nyp, nzm, nzp = neighbours(nu, nxlo, nxhi, nzlo, nzhi, nylo, nyhi, (), x, here)
        nu_up = [0.5 * (here + nxp), 0.5 * (here + nyp), 0.5 * (here + nzp)]
        nu_low = [0.5 * (here + nxm), 0.5 * (here + nym), 0.5 * (here + nzm)]
        centres = [u[c, x] for c in range(3)]
        for c in range(3):
            center = centres[c]
            xm, xp, ym, yp, zm, zp = neighbours(u, xlo, xhi, zlo, zhi, ylo, yhi, (c,), x, center)
            upper = (xp, yp, zp)
            lower = (xm, ym, zm)
            advect = jnp.zeros_like(center)
            spread = jnp.zeros_like(center)
            for d in range(3):
                advect = advect + centres[d] * 0.5 * (upper[d] - lower[d])
                spread = spread + nu_up[d] * (upper[d] - center) - nu_low[d] * (center - lower[d])
            out[c, x] = center + 0.25 * (spread - advect)
        return carry

    lax.fori_loop(0, u.shape[1], plane, 0, unroll=8)


def vmem_call(kernel, out_shape, count, smem=0):
    specs = [pl.BlockSpec(memory_space=pltpu.SMEM)] * smem
    specs += [pl.BlockSpec(memory_space=pltpu.VMEM)] * (count - smem)
    return pl.pallas_call(
        kernel,
        out_shape=out_shape,
        in_specs=specs,
        out_specs=pl.BlockSpec(memory_space=pltpu.VMEM),
        interpret=INTERPRET,
    )


def stencil(velocity, planes, sent):
    u_faces = faces(velocity, 1)
    nu = vmem_call(
        viscosity_kernel, jax.ShapeDtypeStruct(velocity.shape[1:], jnp.float32), 7
    )(velocity, *u_faces)
    nu_faces = faces(nu, 0)
    advanced = vmem_call(advance_kernel, jax.ShapeDtypeStruct(velocity.shape, jnp.float32), 14)(
        velocity, *u_faces, nu, *nu_faces
    )
    slots = sent.shape[0]
    updated = []
    for s in range(slots):
        impulse = jnp.zeros_like(sent[s])
        for t in range(slots):
            impulse = impulse + jnp.where(planes[t] == planes[s], sent[t], 0.0)
        updated.append(lax.dynamic_index_in_dim(advanced, planes[s], 1) + impulse[:, None])
    for s in range(slots):
        advanced = lax.dynamic_update_index_in_dim(advanced, updated[s], planes[s], 1)
    return advanced


def body(velocity, tile_turbine, tile_plane, tile_weight, chord):
    cx = velocity.shape[1]
    vertical_coord = velocity.shape[2]
    spanwise_coord = velocity.shape[3]
    tile_count = tile_turbine.shape[3]
    actuator_count = tile_weight.shape[4]
    nturb = chord.shape[0]
    turbine_list = tile_turbine.reshape(tile_count)
    rotor_planes = tile_plane.reshape(tile_count)
    spread_weights = tile_weight.reshape(
        tile_count, actuator_count, vertical_coord * spanwise_coord
    )
    tiles = jnp.stack(
        [lax.dynamic_index_in_dim(velocity, rotor_planes[s], 1, keepdims=False) for s in range(tile_count)]
    ).reshape(tile_count, 3, vertical_coord * spanwise_coord).astype(jnp.bfloat16)
    block_local = jnp.einsum(
        "spq,scq->scp", spread_weights, tiles, preferred_element_type=jnp.float32
    )
    owning_block = (turbine_list[:, None] == jnp.arange(nturb, dtype=jnp.int32)[None, :]).astype(
        jnp.float32
    )
    partial_sample = jnp.einsum(
        "yr,yw->rw",
        owning_block,
        block_local.reshape(tile_count, -1),
        precision=lax.Precision.HIGHEST,
    )
    rows = lax.axis_size("gx")
    per_row = nturb // rows
    received = lax.all_to_all(
        partial_sample.reshape(rows, per_row, -1), "gx", split_axis=0, concat_axis=0, tiled=True
    )
    owned = jnp.sum(received, axis=0)
    for axis in ("gy", "gz"):
        count = lax.axis_size(axis)
        step = 1
        while step < count:
            pairs = [(i, i ^ step) for i in range(count)]
            owned = owned + lax.ppermute(owned, axis, pairs)
            step *= 2
    owned_coef = lax.dynamic_slice_in_dim(chord, lax.axis_index("gx") * per_row, per_row, 0)
    owned_force = actuate(owned, owned_coef)
    forces = lax.all_to_all(
        jnp.broadcast_to(owned_force[None], (rows,) + owned_force.shape),
        "gx", split_axis=0, concat_axis=0, tiled=True,
    ).reshape(nturb, -1)
    tile_force = jnp.dot(owning_block, forces, precision=lax.Precision.HIGHEST).astype(jnp.bfloat16)
    forces_sent = jnp.einsum(
        "axz,ahx->ahz",
        spread_weights,
        tile_force.reshape(tile_count, 3, actuator_count),
        preferred_element_type=jnp.float32,
    ).reshape(tile_count, 3, vertical_coord, spanwise_coord)
    predicted = stencil(velocity[:, :, :, :], rotor_planes, forces_sent)
    return (predicted, forces)


def solution(mesh):
    placed = (
        P(None, "gx", "gz", "gy"),
        P("gx", "gz", "gy", None),
        P("gx", "gz", "gy", None),
        P("gx", "gz", "gy", None, None, None),
        P(),
    )
    return jax.shard_map(
        body,
        mesh=mesh,
        in_specs=placed,
        out_specs=(P(None, "gx", "gz", "gy"), P()),
        check_vma=False,
    )
```

```python
import jax
import jax.numpy as jnp
from jax import lax
from jax.experimental import pallas as pl
from jax.experimental.pallas import tpu as pltpu
from jax.sharding import PartitionSpec as P

INTERPRET = False


def actuate(velocity_probe, coef):
    rows = velocity_probe.shape[0]
    parts = velocity_probe.reshape(rows, 3, -1)
    magnitude = jnp.sqrt(jnp.sum(parts * parts, axis=1) + 1e-06)
    return (-2.0 * coef[:, None, :] * magnitude[:, None, :] * parts).reshape(rows, -1)


def faces(block, lead):
    ny = block.shape[-1]
    ends = (lax.broadcasted_iota(jnp.int32, (2, ny), 1) == jnp.array([[0], [ny - 1]])).astype(jnp.float32)
    letters = "cxzy"[1 - lead :]
    columns = jnp.einsum(
        letters + ",ky->k" + letters[:-3] + "zx", block, ends, precision=lax.Precision.HIGHEST
    )
    out = []
    for axis, dim in (("gx", lead), ("gz", lead + 1), ("gy", None)):
        count = lax.axis_size(axis)
        forward = [(i, i + 1) for i in range(count - 1)]
        backward = [(target, source) for source, target in forward]
        if dim is None:
            first, last = columns[0], columns[1]
        else:
            size = block.shape[dim]
            first = lax.index_in_dim(block, 0, dim, keepdims=False)
            last = lax.index_in_dim(block, size - 1, dim, keepdims=False)
        out += [lax.ppermute(last, axis, forward), lax.ppermute(first, axis, backward)]
    return out


def neighbours(ref, xlo, xhi, zlo, zhi, ylo, yhi, lead, x, centre):
    nx = ref.shape[-3]
    nz, ny = centre.shape
    sub = lax.broadcasted_iota(jnp.int32, (nz, ny), 0)
    lane = lax.broadcasted_iota(jnp.int32, (nz, ny), 1)
    column = lax.broadcasted_iota(jnp.int32, (nz, nx), 1)
    prev = ref[lead + (jnp.maximum(x - 1, 0),)]
    nxt = ref[lead + (jnp.minimum(x + 1, nx - 1),)]
    xm = jnp.where(x == 0, xlo[lead], prev)
    xp = jnp.where(x == nx - 1, xhi[lead], nxt)
    zl = zlo[lead + (pl.ds(x, 1), slice(None))]
    zh = zhi[lead + (pl.ds(x, 1), slice(None))]
    zm = jnp.where(sub == 0, zl, pltpu.roll(centre, 1, 0))
    zp = jnp.where(sub == nz - 1, zh, pltpu.roll(centre, nz - 1, 0))
    yl = jnp.sum(jnp.where(column == x, ylo[lead], 0.0), axis=1, keepdims=True)
    yh = jnp.sum(jnp.where(column == x, yhi[lead], 0.0), axis=1, keepdims=True)
    ym = jnp.where(lane == 0, yl, pltpu.roll(centre, 1, 1))
    yp = jnp.where(lane == ny - 1, yh, pltpu.roll(centre, ny - 1, 1))
    return xm, xp, ym, yp, zm, zp


def viscosity_kernel(u, xlo, xhi, zlo, zhi, ylo, yhi, nu):
    def plane(x, carry):
        diffs = []
        for c in range(3):
            xm, xp, ym, yp, zm, zp = neighbours(u, xlo, xhi, zlo, zhi, ylo, yhi, (c,), x, u[c, x])
            diffs.append([xp - xm, yp - ym, zp - zm])
        diagonal = None
        for c in range(3):
            strain = 0.5 * diffs[c][c]
            diagonal = strain * strain if diagonal is None else diagonal + strain * strain
        cross = None
        for c in range(3):
            for d in range(c + 1, 3):
                strain = 0.25 * (diffs[c][d] + diffs[d][c])
                cross = strain * strain if cross is None else cross + strain * strain
        total = diagonal + 2.0 * cross
        nu[x] = 0.05 + 1.0 * jnp.sqrt(2.0 * total + 1e-06)
        return carry

    lax.fori_loop(0, u.shape[1], plane, 0, unroll=8)


def advance_kernel(planes, u, xlo, xhi, zlo, zhi, ylo, yhi, nu, nxlo, nxhi, nzlo, nzhi, nylo, nyhi, sent, out):
    slots = sent.shape[0]

    def plane(x, carry):
        here = nu[x]
        nxm, nxp, nym, nyp, nzm, nzp = neighbours(nu, nxlo, nxhi, nzlo, nzhi, nylo, nyhi, (), x, here)
        nu_up = [here + nxp, here + nyp, here + nzp]
        nu_low = [here + nxm, here + nym, here + nzm]
        centres = [u[c, x] for c in range(3)]
        for c in range(3):
            center = centres[c]
            xm, xp, ym, yp, zm, zp = neighbours(u, xlo, xhi, zlo, zhi, ylo, yhi, (c,), x, center)
            upper = (xp, yp, zp)
            lower = (xm, ym, zm)
            advect = None
            spread = None
            for d in range(3):
                term = centres[d] * (upper[d] - lower[d])
                flux = nu_up[d] * (upper[d] - center) - nu_low[d] * (center - lower[d])
                advect = term if advect is None else advect + term
                spread = flux if spread is None else spread + flux
            impulse = jnp.zeros_like(center)
            for s in range(slots):
                impulse = impulse + jnp.where(planes[s] == x, sent[s, c], 0.0)
            out[c, x] = center + 0.125 * (spread - advect) + impulse
        return carry

    lax.fori_loop(0, u.shape[1], plane, 0, unroll=8)


def vmem_call(kernel, out_shape, count, smem=0):
    specs = [pl.BlockSpec(memory_space=pltpu.SMEM)] * smem
    specs += [pl.BlockSpec(memory_space=pltpu.VMEM)] * (count - smem)
    return pl.pallas_call(
        kernel,
        out_shape=out_shape,
        in_specs=specs,
        out_specs=pl.BlockSpec(memory_space=pltpu.VMEM),
        interpret=INTERPRET,
    )


def stencil(velocity, planes, sent):
    u_faces = faces(velocity, 1)
    nu = vmem_call(
        viscosity_kernel, jax.ShapeDtypeStruct(velocity.shape[1:], jnp.float32), 7
    )(velocity, *u_faces)
    nu_faces = faces(nu, 0)
    return vmem_call(
        advance_kernel, jax.ShapeDtypeStruct(velocity.shape, jnp.float32), 16, smem=1
    )(planes, velocity, *u_faces, nu, *nu_faces, sent)


def body(velocity, tile_turbine, tile_plane, tile_weight, chord):
    cx = velocity.shape[1]
    vertical_coord = velocity.shape[2]
    spanwise_coord = velocity.shape[3]
    tile_count = tile_turbine.shape[3]
    actuator_count = tile_weight.shape[4]
    nturb = chord.shape[0]
    turbine_list = tile_turbine.reshape(tile_count)
    rotor_planes = tile_plane.reshape(tile_count)
    spread_weights = tile_weight.reshape(
        tile_count, actuator_count, vertical_coord * spanwise_coord
    )
    tiles = jnp.stack(
        [lax.dynamic_index_in_dim(velocity, rotor_planes[s], 1, keepdims=False) for s in range(tile_count)]
    ).reshape(tile_count, 3, vertical_coord * spanwise_coord).astype(jnp.bfloat16)
    block_local = jnp.einsum(
        "spq,scq->scp", spread_weights, tiles, preferred_element_type=jnp.float32
    )
    owning_block = (turbine_list[:, None] == jnp.arange(nturb, dtype=jnp.int32)[None, :]).astype(
        jnp.float32
    )
    partial_sample = jnp.einsum(
        "yr,yw->rw",
        owning_block,
        block_local.reshape(tile_count, -1),
        precision=lax.Precision.HIGHEST,
    )
    rows = lax.axis_size("gx")
    per_row = nturb // rows
    received = lax.all_to_all(
        partial_sample.reshape(rows, per_row, -1), "gx", split_axis=0, concat_axis=0, tiled=True
    )
    owned = jnp.sum(received, axis=0)
    for axis in ("gy", "gz"):
        count = lax.axis_size(axis)
        step = 1
        while step < count:
            pairs = [(i, i ^ step) for i in range(count)]
            owned = owned + lax.ppermute(owned, axis, pairs)
            step *= 2
    owned_coef = lax.dynamic_slice_in_dim(chord, lax.axis_index("gx") * per_row, per_row, 0)
    owned_force = actuate(owned, owned_coef)
    forces = lax.all_to_all(
        jnp.broadcast_to(owned_force[None], (rows,) + owned_force.shape),
        "gx", split_axis=0, concat_axis=0, tiled=True,
    ).reshape(nturb, -1)
    tile_force = jnp.dot(owning_block, forces, precision=lax.Precision.HIGHEST).astype(jnp.bfloat16)
    forces_sent = jnp.einsum(
        "axz,ahx->ahz",
        spread_weights,
        tile_force.reshape(tile_count, 3, actuator_count),
        preferred_element_type=jnp.float32,
    ).reshape(tile_count, 3, vertical_coord, spanwise_coord)
    predicted = stencil(velocity[:, :, :, :], rotor_planes, forces_sent)
    return (predicted, forces)


def solution(mesh):
    placed = (
        P(None, "gx", "gz", "gy"),
        P("gx", "gz", "gy", None),
        P("gx", "gz", "gy", None),
        P("gx", "gz", "gy", None, None, None),
        P(),
    )
    return jax.shard_map(
        body,
        mesh=mesh,
        in_specs=placed,
        out_specs=(P(None, "gx", "gz", "gy"), P()),
        check_vma=False,
    )
```

```python
import jax
import jax.numpy as jnp
from jax import lax
from jax.experimental import pallas as pl
from jax.experimental.pallas import tpu as pltpu
from jax.sharding import PartitionSpec as P

INTERPRET = False


def actuate(velocity_probe, coef):
    rows = velocity_probe.shape[0]
    parts = velocity_probe.reshape(rows, 3, -1)
    magnitude = jnp.sqrt(jnp.sum(parts * parts, axis=1) + 1e-06)
    return (-2.0 * coef[:, None, :] * magnitude[:, None, :] * parts).reshape(rows, -1)


def faces(block, lead):
    ny = block.shape[-1]
    ends = (lax.broadcasted_iota(jnp.int32, (2, ny), 1) == jnp.array([[0], [ny - 1]])).astype(jnp.float32)
    letters = "cxzy"[1 - lead :]
    columns = jnp.einsum(
        letters + ",ky->k" + letters[:-3] + "zx", block, ends, precision=lax.Precision.HIGHEST
    )
    out = []
    for axis, dim in (("gx", lead), ("gz", lead + 1), ("gy", None)):
        count = lax.axis_size(axis)
        forward = [(i, i + 1) for i in range(count - 1)]
        backward = [(target, source) for source, target in forward]
        if dim is None:
            pad = [(0, 0)] * (columns.ndim - 2) + [(0, ny - columns.shape[-1])]
            first, last = jnp.pad(columns[0], pad), jnp.pad(columns[1], pad)
        else:
            size = block.shape[dim]
            first = lax.index_in_dim(block, 0, dim, keepdims=False)
            last = lax.index_in_dim(block, size - 1, dim, keepdims=False)
        out += [lax.ppermute(last, axis, forward), lax.ppermute(first, axis, backward)]
    return out


def neighbours(ref, xlo, xhi, zlo, zhi, ylo, yhi, lead, x, centre):
    nx = ref.shape[-3]
    nz, ny = centre.shape
    sub = lax.broadcasted_iota(jnp.int32, (nz, ny), 0)
    lane = lax.broadcasted_iota(jnp.int32, (nz, ny), 1)
    prev = ref[lead + (jnp.maximum(x - 1, 0),)]
    nxt = ref[lead + (jnp.minimum(x + 1, nx - 1),)]
    xm = jnp.where(x == 0, xlo[lead], prev)
    xp = jnp.where(x == nx - 1, xhi[lead], nxt)
    zl = zlo[lead + (pl.ds(x, 1), slice(None))]
    zh = zhi[lead + (pl.ds(x, 1), slice(None))]
    zm = jnp.where(sub == 0, zl, pltpu.roll(centre, 1, 0))
    zp = jnp.where(sub == nz - 1, zh, pltpu.roll(centre, nz - 1, 0))
    yl = pltpu.roll(ylo[lead], jnp.where(x == 0, 0, ny - x), 1)
    yh = pltpu.roll(yhi[lead], ny - 1 - x, 1)
    ym = jnp.where(lane == 0, yl, pltpu.roll(centre, 1, 1))
    yp = jnp.where(lane == ny - 1, yh, pltpu.roll(centre, ny - 1, 1))
    return xm, xp, ym, yp, zm, zp


def viscosity_kernel(u, xlo, xhi, zlo, zhi, ylo, yhi, nu):
    def plane(x, carry):
        diffs = []
        for c in range(3):
            xm, xp, ym, yp, zm, zp = neighbours(u, xlo, xhi, zlo, zhi, ylo, yhi, (c,), x, u[c, x])
            diffs.append([xp - xm, yp - ym, zp - zm])
        diagonal = None
        for c in range(3):
            strain = 0.5 * diffs[c][c]
            diagonal = strain * strain if diagonal is None else diagonal + strain * strain
        cross = None
        for c in range(3):
            for d in range(c + 1, 3):
                strain = 0.25 * (diffs[c][d] + diffs[d][c])
                cross = strain * strain if cross is None else cross + strain * strain
        total = diagonal + 2.0 * cross
        nu[x] = 0.05 + 1.0 * jnp.sqrt(2.0 * total + 1e-06)
        return carry

    lax.fori_loop(0, u.shape[1], plane, 0, unroll=8)


def advance_kernel(planes, u, xlo, xhi, zlo, zhi, ylo, yhi, nu, nxlo, nxhi, nzlo, nzhi, nylo, nyhi, sent, out):
    slots = sent.shape[0]

    def plane(x, carry):
        here = nu[x]
        nxm, nxp, nym, nyp, nzm, nzp = neighbours(nu, nxlo, nxhi, nzlo, nzhi, nylo, nyhi, (), x, here)
        nu_up = [here + nxp, here + nyp, here + nzp]
        nu_low = [here + nxm, here + nym, here + nzm]
        centres = [u[c, x] for c in range(3)]
        for c in range(3):
            center = centres[c]
            xm, xp, ym, yp, zm, zp = neighbours(u, xlo, xhi, zlo, zhi, ylo, yhi, (c,), x, center)
            upper = (xp, yp, zp)
            lower = (xm, ym, zm)
            advect = None
            spread = None
            for d in range(3):
                term = centres[d] * (upper[d] - lower[d])
                flux = nu_up[d] * (upper[d] - center) - nu_low[d] * (center - lower[d])
                advect = term if advect is None else advect + term
                spread = flux if spread is None else spread + flux
            impulse = jnp.zeros_like(center)
            for s in range(slots):
                impulse = impulse + jnp.where(planes[s] == x, sent[s, c], 0.0)
            out[c, x] = center + 0.125 * (spread - advect) + impulse
        return carry

    lax.fori_loop(0, u.shape[1], plane, 0, unroll=8)


def vmem_call(kernel, out_shape, count, smem=0):
    specs = [pl.BlockSpec(memory_space=pltpu.SMEM)] * smem
    specs += [pl.BlockSpec(memory_space=pltpu.VMEM)] * (count - smem)
    return pl.pallas_call(
        kernel,
        out_shape=out_shape,
        in_specs=specs,
        out_specs=pl.BlockSpec(memory_space=pltpu.VMEM),
        interpret=INTERPRET,
    )


def stencil(velocity, planes, sent):
    u_faces = faces(velocity, 1)
    nu = vmem_call(
        viscosity_kernel, jax.ShapeDtypeStruct(velocity.shape[1:], jnp.float32), 7
    )(velocity, *u_faces)
    nu_faces = faces(nu, 0)
    return vmem_call(
        advance_kernel, jax.ShapeDtypeStruct(velocity.shape, jnp.float32), 16, smem=1
    )(planes, velocity, *u_faces, nu, *nu_faces, sent)


def body(velocity, tile_turbine, tile_plane, tile_weight, chord):
    cx = velocity.shape[1]
    vertical_coord = velocity.shape[2]
    spanwise_coord = velocity.shape[3]
    tile_count = tile_turbine.shape[3]
    actuator_count = tile_weight.shape[4]
    nturb = chord.shape[0]
    turbine_list = tile_turbine.reshape(tile_count)
    rotor_planes = tile_plane.reshape(tile_count)
    spread_weights = tile_weight.reshape(
        tile_count, actuator_count, vertical_coord * spanwise_coord
    )
    tiles = jnp.stack(
        [lax.dynamic_index_in_dim(velocity, rotor_planes[s], 1, keepdims=False) for s in range(tile_count)]
    ).reshape(tile_count, 3, vertical_coord * spanwise_coord).astype(jnp.bfloat16)
    block_local = jnp.einsum(
        "spq,scq->scp", spread_weights, tiles, preferred_element_type=jnp.float32
    )
    owning_block = (turbine_list[:, None] == jnp.arange(nturb, dtype=jnp.int32)[None, :]).astype(
        jnp.float32
    )
    partial_sample = jnp.einsum(
        "yr,yw->rw",
        owning_block,
        block_local.reshape(tile_count, -1),
        precision=lax.Precision.HIGHEST,
    )
    rows = lax.axis_size("gx")
    per_row = nturb // rows
    received = lax.all_to_all(
        partial_sample.reshape(rows, per_row, -1), "gx", split_axis=0, concat_axis=0, tiled=True
    )
    owned = jnp.sum(received, axis=0)
    for axis in ("gy", "gz"):
        count = lax.axis_size(axis)
        step = 1
        while step < count:
            pairs = [(i, i ^ step) for i in range(count)]
            owned = owned + lax.ppermute(owned, axis, pairs)
            step *= 2
    owned_coef = lax.dynamic_slice_in_dim(chord, lax.axis_index("gx") * per_row, per_row, 0)
    owned_force = actuate(owned, owned_coef)
    forces = lax.all_to_all(
        jnp.broadcast_to(owned_force[None], (rows,) + owned_force.shape),
        "gx", split_axis=0, concat_axis=0, tiled=True,
    ).reshape(nturb, -1)
    tile_force = jnp.dot(owning_block, forces, precision=lax.Precision.HIGHEST).astype(jnp.bfloat16)
    forces_sent = jnp.einsum(
        "axz,ahx->ahz",
        spread_weights,
        tile_force.reshape(tile_count, 3, actuator_count),
        preferred_element_type=jnp.float32,
    ).reshape(tile_count, 3, vertical_coord, spanwise_coord)
    predicted = stencil(velocity[:, :, :, :], rotor_planes, forces_sent)
    return (predicted, forces)


def solution(mesh):
    placed = (
        P(None, "gx", "gz", "gy"),
        P("gx", "gz", "gy", None),
        P("gx", "gz", "gy", None),
        P("gx", "gz", "gy", None, None, None),
        P(),
    )
    return jax.shard_map(
        body,
        mesh=mesh,
        in_specs=placed,
        out_specs=(P(None, "gx", "gz", "gy"), P()),
        check_vma=False,
    )
```

```python
import jax
import jax.numpy as jnp
from jax import lax
from jax.experimental import pallas as pl
from jax.experimental.pallas import tpu as pltpu
from jax.sharding import PartitionSpec as P

INTERPRET = False


def actuate(velocity_probe, coef):
    rows = velocity_probe.shape[0]
    parts = velocity_probe.reshape(rows, 3, -1)
    magnitude = jnp.sqrt(jnp.sum(parts * parts, axis=1) + 1e-06)
    return (-2.0 * coef[:, None, :] * magnitude[:, None, :] * parts).reshape(rows, -1)


def faces(block, lead):
    ny = block.shape[-1]
    if lead:
        ends = (lax.broadcasted_iota(jnp.int32, (2, ny), 1) == jnp.array([[0], [ny - 1]])).astype(jnp.float32)
        columns = jnp.einsum("cxzy,ky->kczx", block, ends, precision=lax.Precision.HIGHEST)
    else:
        lane = lax.broadcasted_iota(jnp.int32, block.shape, block.ndim - 1)
        columns = jnp.stack(
            [jnp.swapaxes(jnp.sum(jnp.where(lane == y, block, 0.0), axis=-1), -1, -2) for y in (0, ny - 1)]
        )
    out = []
    for axis, dim in (("gx", lead), ("gz", lead + 1), ("gy", None)):
        count = lax.axis_size(axis)
        forward = [(i, i + 1) for i in range(count - 1)]
        backward = [(target, source) for source, target in forward]
        if dim is None:
            pad = [(0, 0)] * (columns.ndim - 2) + [(0, ny - columns.shape[-1])]
            first, last = jnp.pad(columns[0], pad), jnp.pad(columns[1], pad)
        else:
            size = block.shape[dim]
            first = lax.index_in_dim(block, 0, dim, keepdims=False)
            last = lax.index_in_dim(block, size - 1, dim, keepdims=False)
        out += [lax.ppermute(last, axis, forward), lax.ppermute(first, axis, backward)]
    return out


def neighbours(ref, xlo, xhi, zlo, zhi, ylo, yhi, lead, x, centre):
    nx = ref.shape[-3]
    nz, ny = centre.shape
    sub = lax.broadcasted_iota(jnp.int32, (nz, ny), 0)
    lane = lax.broadcasted_iota(jnp.int32, (nz, ny), 1)
    prev = ref[lead + (jnp.maximum(x - 1, 0),)]
    nxt = ref[lead + (jnp.minimum(x + 1, nx - 1),)]
    xm = jnp.where(x == 0, xlo[lead], prev)
    xp = jnp.where(x == nx - 1, xhi[lead], nxt)
    zl = zlo[lead + (pl.ds(x, 1), slice(None))]
    zh = zhi[lead + (pl.ds(x, 1), slice(None))]
    zm = jnp.where(sub == 0, zl, pltpu.roll(centre, 1, 0))
    zp = jnp.where(sub == nz - 1, zh, pltpu.roll(centre, nz - 1, 0))
    yl = pltpu.roll(ylo[lead], jnp.where(x == 0, 0, ny - x), 1)
    yh = pltpu.roll(yhi[lead], ny - 1 - x, 1)
    ym = jnp.where(lane == 0, yl, pltpu.roll(centre, 1, 1))
    yp = jnp.where(lane == ny - 1, yh, pltpu.roll(centre, ny - 1, 1))
    return xm, xp, ym, yp, zm, zp


def viscosity_kernel(u, xlo, xhi, zlo, zhi, ylo, yhi, nu):
    def plane(x, carry):
        diffs = []
        for c in range(3):
            xm, xp, ym, yp, zm, zp = neighbours(u, xlo, xhi, zlo, zhi, ylo, yhi, (c,), x, u[c, x])
            diffs.append([xp - xm, yp - ym, zp - zm])
        diagonal = None
        for c in range(3):
            strain = 0.5 * diffs[c][c]
            diagonal = strain * strain if diagonal is None else diagonal + strain * strain
        cross = None
        for c in range(3):
            for d in range(c + 1, 3):
                strain = 0.25 * (diffs[c][d] + diffs[d][c])
                cross = strain * strain if cross is None else cross + strain * strain
        total = diagonal + 2.0 * cross
        nu[x] = 0.05 + 1.0 * jnp.sqrt(2.0 * total + 1e-06)
        return carry

    lax.fori_loop(0, u.shape[1], plane, 0, unroll=8)


def advance_kernel(planes, u, xlo, xhi, zlo, zhi, ylo, yhi, nu, nxlo, nxhi, nzlo, nzhi, nylo, nyhi, sent, out):
    slots = sent.shape[0]

    def plane(x, carry):
        here = nu[x]
        nxm, nxp, nym, nyp, nzm, nzp = neighbours(nu, nxlo, nxhi, nzlo, nzhi, nylo, nyhi, (), x, here)
        nu_up = [here + nxp, here + nyp, here + nzp]
        nu_low = [here + nxm, here + nym, here + nzm]
        centres = [u[c, x] for c in range(3)]
        for c in range(3):
            center = centres[c]
            xm, xp, ym, yp, zm, zp = neighbours(u, xlo, xhi, zlo, zhi, ylo, yhi, (c,), x, center)
            upper = (xp, yp, zp)
            lower = (xm, ym, zm)
            advect = None
            spread = None
            for d in range(3):
                term = centres[d] * (upper[d] - lower[d])
                flux = nu_up[d] * (upper[d] - center) - nu_low[d] * (center - lower[d])
                advect = term if advect is None else advect + term
                spread = flux if spread is None else spread + flux
            impulse = jnp.zeros_like(center)
            for s in range(slots):
                impulse = impulse + jnp.where(planes[s] == x, sent[s, c], 0.0)
            out[c, x] = center + 0.125 * (spread - advect) + impulse
        return carry

    lax.fori_loop(0, u.shape[1], plane, 0, unroll=8)


def vmem_call(kernel, out_shape, count, smem=0):
    specs = [pl.BlockSpec(memory_space=pltpu.SMEM)] * smem
    specs += [pl.BlockSpec(memory_space=pltpu.VMEM)] * (count - smem)
    return pl.pallas_call(
        kernel,
        out_shape=out_shape,
        in_specs=specs,
        out_specs=pl.BlockSpec(memory_space=pltpu.VMEM),
        interpret=INTERPRET,
    )


def stencil(velocity, planes, sent):
    u_faces = faces(velocity, 1)
    nu = vmem_call(
        viscosity_kernel, jax.ShapeDtypeStruct(velocity.shape[1:], jnp.float32), 7
    )(velocity, *u_faces)
    nu_faces = faces(nu, 0)
    return vmem_call(
        advance_kernel, jax.ShapeDtypeStruct(velocity.shape, jnp.float32), 16, smem=1
    )(planes, velocity, *u_faces, nu, *nu_faces, sent)


def body(velocity, tile_turbine, tile_plane, tile_weight, chord):
    cx = velocity.shape[1]
    vertical_coord = velocity.shape[2]
    spanwise_coord = velocity.shape[3]
    tile_count = tile_turbine.shape[3]
    actuator_count = tile_weight.shape[4]
    nturb = chord.shape[0]
    turbine_list = tile_turbine.reshape(tile_count)
    rotor_planes = tile_plane.reshape(tile_count)
    spread_weights = tile_weight.reshape(
        tile_count, actuator_count, vertical_coord * spanwise_coord
    )
    tiles = jnp.stack(
        [lax.dynamic_index_in_dim(velocity, rotor_planes[s], 1, keepdims=False) for s in range(tile_count)]
    ).reshape(tile_count, 3, vertical_coord * spanwise_coord).astype(jnp.bfloat16)
    block_local = jnp.einsum(
        "spq,scq->scp", spread_weights, tiles, preferred_element_type=jnp.float32
    )
    owning_block = (turbine_list[:, None] == jnp.arange(nturb, dtype=jnp.int32)[None, :]).astype(
        jnp.float32
    )
    partial_sample = jnp.einsum(
        "yr,yw->rw",
        owning_block,
        block_local.reshape(tile_count, -1),
        precision=lax.Precision.HIGHEST,
    )
    rows = lax.axis_size("gx")
    per_row = nturb // rows
    received = lax.all_to_all(
        partial_sample.reshape(rows, per_row, -1), "gx", split_axis=0, concat_axis=0, tiled=True
    )
    owned = jnp.sum(received, axis=0)
    for axis in ("gy", "gz"):
        count = lax.axis_size(axis)
        step = 1
        while step < count:
            pairs = [(i, i ^ step) for i in range(count)]
            owned = owned + lax.ppermute(owned, axis, pairs)
            step *= 2
    owned_coef = lax.dynamic_slice_in_dim(chord, lax.axis_index("gx") * per_row, per_row, 0)
    owned_force = actuate(owned, owned_coef)
    forces = lax.all_to_all(
        jnp.broadcast_to(owned_force[None], (rows,) + owned_force.shape),
        "gx", split_axis=0, concat_axis=0, tiled=True,
    ).reshape(nturb, -1)
    tile_force = jnp.dot(owning_block, forces, precision=lax.Precision.HIGHEST).astype(jnp.bfloat16)
    forces_sent = jnp.einsum(
        "axz,ahx->ahz",
        spread_weights,
        tile_force.reshape(tile_count, 3, actuator_count),
        preferred_element_type=jnp.float32,
    ).reshape(tile_count, 3, vertical_coord, spanwise_coord)
    predicted = stencil(velocity[:, :, :, :], rotor_planes, forces_sent)
    return (predicted, forces)


def solution(mesh):
    placed = (
        P(None, "gx", "gz", "gy"),
        P("gx", "gz", "gy", None),
        P("gx", "gz", "gy", None),
        P("gx", "gz", "gy", None, None, None),
        P(),
    )
    return jax.shard_map(
        body,
        mesh=mesh,
        in_specs=placed,
        out_specs=(P(None, "gx", "gz", "gy"), P()),
        check_vma=False,
    )
```

```python
import jax
import jax.numpy as jnp
from jax import lax
from jax.experimental import pallas as pl
from jax.experimental.pallas import tpu as pltpu
from jax.sharding import PartitionSpec as P

INTERPRET = False


def actuate(velocity_probe, coef):
    rows = velocity_probe.shape[0]
    parts = velocity_probe.reshape(rows, 3, -1)
    magnitude = jnp.sqrt(jnp.sum(parts * parts, axis=1) + 1e-06)
    return (-2.0 * coef[:, None, :] * magnitude[:, None, :] * parts).reshape(rows, -1)


def faces(block, lead):
    ny = block.shape[-1]
    if lead:
        ends = (lax.broadcasted_iota(jnp.int32, (2, ny), 1) == jnp.array([[0], [ny - 1]])).astype(jnp.float32)
        columns = jnp.einsum("cxzy,ky->kczx", block, ends, precision=lax.Precision.HIGHEST)
    else:
        lane = lax.broadcasted_iota(jnp.int32, block.shape, block.ndim - 1)
        columns = jnp.stack(
            [jnp.swapaxes(jnp.sum(jnp.where(lane == y, block, 0.0), axis=-1), -1, -2) for y in (0, ny - 1)]
        )
    out = []
    for axis, dim in (("gx", lead), ("gz", lead + 1), ("gy", None)):
        count = lax.axis_size(axis)
        forward = [(i, i + 1) for i in range(count - 1)]
        backward = [(target, source) for source, target in forward]
        if dim is None:
            pad = [(0, 0)] * (columns.ndim - 2) + [(0, ny - columns.shape[-1])]
            first, last = jnp.pad(columns[0], pad), jnp.pad(columns[1], pad)
        else:
            size = block.shape[dim]
            first = lax.index_in_dim(block, 0, dim, keepdims=False)
            last = lax.index_in_dim(block, size - 1, dim, keepdims=False)
        out += [lax.ppermute(last, axis, forward), lax.ppermute(first, axis, backward)]
    return out


def neighbours(ref, xlo, xhi, zlo, zhi, ylo, yhi, lead, x, centre):
    nx = ref.shape[-3]
    nz, ny = centre.shape
    sub = lax.broadcasted_iota(jnp.int32, (nz, ny), 0)
    lane = lax.broadcasted_iota(jnp.int32, (nz, ny), 1)
    prev = ref[lead + (jnp.maximum(x - 1, 0),)]
    nxt = ref[lead + (jnp.minimum(x + 1, nx - 1),)]
    xm = jnp.where(x == 0, xlo[lead], prev)
    xp = jnp.where(x == nx - 1, xhi[lead], nxt)
    zl = zlo[lead + (pl.ds(x, 1), slice(None))]
    zh = zhi[lead + (pl.ds(x, 1), slice(None))]
    zm = jnp.where(sub == 0, zl, pltpu.roll(centre, 1, 0))
    zp = jnp.where(sub == nz - 1, zh, pltpu.roll(centre, nz - 1, 0))
    yl = pltpu.roll(ylo[lead], jnp.where(x == 0, 0, ny - x), 1)
    yh = pltpu.roll(yhi[lead], ny - 1 - x, 1)
    ym = jnp.where(lane == 0, yl, pltpu.roll(centre, 1, 1))
    yp = jnp.where(lane == ny - 1, yh, pltpu.roll(centre, ny - 1, 1))
    return xm, xp, ym, yp, zm, zp


def viscosity_kernel(u, xlo, xhi, zlo, zhi, ylo, yhi, nu):
    def plane(x, carry):
        diffs = []
        for c in range(3):
            xm, xp, ym, yp, zm, zp = neighbours(u, xlo, xhi, zlo, zhi, ylo, yhi, (c,), x, u[c, x])
            diffs.append([xp - xm, yp - ym, zp - zm])
        diagonal = None
        for c in range(3):
            strain = 0.5 * diffs[c][c]
            diagonal = strain * strain if diagonal is None else diagonal + strain * strain
        cross = None
        for c in range(3):
            for d in range(c + 1, 3):
                strain = 0.25 * (diffs[c][d] + diffs[d][c])
                cross = strain * strain if cross is None else cross + strain * strain
        total = diagonal + 2.0 * cross
        nu[x] = 0.05 + 1.0 * jnp.sqrt(2.0 * total + 1e-06)
        return carry

    lax.fori_loop(0, u.shape[1], plane, 0, unroll=16)


def advance_kernel(planes, u, xlo, xhi, zlo, zhi, ylo, yhi, nu, nxlo, nxhi, nzlo, nzhi, nylo, nyhi, sent, out):
    slots = sent.shape[0]

    def plane(x, carry):
        here = nu[x]
        nxm, nxp, nym, nyp, nzm, nzp = neighbours(nu, nxlo, nxhi, nzlo, nzhi, nylo, nyhi, (), x, here)
        nu_up = [here + nxp, here + nyp, here + nzp]
        nu_low = [here + nxm, here + nym, here + nzm]
        centres = [u[c, x] for c in range(3)]
        for c in range(3):
            center = centres[c]
            xm, xp, ym, yp, zm, zp = neighbours(u, xlo, xhi, zlo, zhi, ylo, yhi, (c,), x, center)
            upper = (xp, yp, zp)
            lower = (xm, ym, zm)
            advect = None
            spread = None
            for d in range(3):
                term = centres[d] * (upper[d] - lower[d])
                flux = nu_up[d] * (upper[d] - center) - nu_low[d] * (center - lower[d])
                advect = term if advect is None else advect + term
                spread = flux if spread is None else spread + flux
            impulse = jnp.zeros_like(center)
            for s in range(slots):
                impulse = impulse + jnp.where(planes[s] == x, sent[s, c], 0.0)
            out[c, x] = center + 0.125 * (spread - advect) + impulse
        return carry

    lax.fori_loop(0, u.shape[1], plane, 0, unroll=16)


def vmem_call(kernel, out_shape, count, smem=0):
    specs = [pl.BlockSpec(memory_space=pltpu.SMEM)] * smem
    specs += [pl.BlockSpec(memory_space=pltpu.VMEM)] * (count - smem)
    return pl.pallas_call(
        kernel,
        out_shape=out_shape,
        in_specs=specs,
        out_specs=pl.BlockSpec(memory_space=pltpu.VMEM),
        interpret=INTERPRET,
    )


def stencil(velocity, planes, sent):
    u_faces = faces(velocity, 1)
    nu = vmem_call(
        viscosity_kernel, jax.ShapeDtypeStruct(velocity.shape[1:], jnp.float32), 7
    )(velocity, *u_faces)
    nu_faces = faces(nu, 0)
    return vmem_call(
        advance_kernel, jax.ShapeDtypeStruct(velocity.shape, jnp.float32), 16, smem=1
    )(planes, velocity, *u_faces, nu, *nu_faces, sent)


def body(velocity, tile_turbine, tile_plane, tile_weight, chord):
    cx = velocity.shape[1]
    vertical_coord = velocity.shape[2]
    spanwise_coord = velocity.shape[3]
    tile_count = tile_turbine.shape[3]
    actuator_count = tile_weight.shape[4]
    nturb = chord.shape[0]
    turbine_list = tile_turbine.reshape(tile_count)
    rotor_planes = tile_plane.reshape(tile_count)
    spread_weights = tile_weight.reshape(
        tile_count, actuator_count, vertical_coord * spanwise_coord
    )
    tiles = jnp.stack(
        [lax.dynamic_index_in_dim(velocity, rotor_planes[s], 1, keepdims=False) for s in range(tile_count)]
    ).reshape(tile_count, 3, vertical_coord * spanwise_coord).astype(jnp.bfloat16)
    block_local = jnp.einsum(
        "spq,scq->scp", spread_weights, tiles, preferred_element_type=jnp.float32
    )
    owning_block = (turbine_list[:, None] == jnp.arange(nturb, dtype=jnp.int32)[None, :]).astype(
        jnp.float32
    )
    partial_sample = jnp.einsum(
        "yr,yw->rw",
        owning_block,
        block_local.reshape(tile_count, -1),
        precision=lax.Precision.HIGHEST,
    )
    rows = lax.axis_size("gx")
    per_row = nturb // rows
    received = lax.all_to_all(
        partial_sample.reshape(rows, per_row, -1), "gx", split_axis=0, concat_axis=0, tiled=True
    )
    owned = jnp.sum(received, axis=0)
    for axis in ("gy", "gz"):
        count = lax.axis_size(axis)
        step = 1
        while step < count:
            pairs = [(i, i ^ step) for i in range(count)]
            owned = owned + lax.ppermute(owned, axis, pairs)
            step *= 2
    owned_coef = lax.dynamic_slice_in_dim(chord, lax.axis_index("gx") * per_row, per_row, 0)
    owned_force = actuate(owned, owned_coef)
    forces = lax.all_to_all(
        jnp.broadcast_to(owned_force[None], (rows,) + owned_force.shape),
        "gx", split_axis=0, concat_axis=0, tiled=True,
    ).reshape(nturb, -1)
    tile_force = jnp.dot(owning_block, forces, precision=lax.Precision.HIGHEST).astype(jnp.bfloat16)
    forces_sent = jnp.einsum(
        "axz,ahx->ahz",
        spread_weights,
        tile_force.reshape(tile_count, 3, actuator_count),
        preferred_element_type=jnp.float32,
    ).reshape(tile_count, 3, vertical_coord, spanwise_coord)
    predicted = stencil(velocity[:, :, :, :], rotor_planes, forces_sent)
    return (predicted, forces)


def solution(mesh):
    placed = (
        P(None, "gx", "gz", "gy"),
        P("gx", "gz", "gy", None),
        P("gx", "gz", "gy", None),
        P("gx", "gz", "gy", None, None, None),
        P(),
    )
    return jax.shard_map(
        body,
        mesh=mesh,
        in_specs=placed,
        out_specs=(P(None, "gx", "gz", "gy"), P()),
        check_vma=False,
    )
```

```python
import jax
import jax.numpy as jnp
from jax import lax
from jax.experimental import pallas as pl
from jax.experimental.pallas import tpu as pltpu
from jax.sharding import PartitionSpec as P

INTERPRET = False


def actuate(velocity_probe, coef):
    rows = velocity_probe.shape[0]
    parts = velocity_probe.reshape(rows, 3, -1)
    magnitude = jnp.sqrt(jnp.sum(parts * parts, axis=1) + 1e-06)
    return (-2.0 * coef[:, None, :] * magnitude[:, None, :] * parts).reshape(rows, -1)


def faces(block, lead):
    ny = block.shape[-1]
    if lead:
        ends = (lax.broadcasted_iota(jnp.int32, (2, ny), 1) == jnp.array([[0], [ny - 1]])).astype(jnp.float32)
        columns = jnp.einsum("cxzy,ky->kczx", block, ends, precision=lax.Precision.HIGHEST)
    else:
        lane = lax.broadcasted_iota(jnp.int32, block.shape, block.ndim - 1)
        columns = jnp.stack(
            [jnp.swapaxes(jnp.sum(jnp.where(lane == y, block, 0.0), axis=-1), -1, -2) for y in (0, ny - 1)]
        )
    out = []
    for axis, dim in (("gx", lead), ("gz", lead + 1), ("gy", None)):
        count = lax.axis_size(axis)
        forward = [(i, i + 1) for i in range(count - 1)]
        backward = [(target, source) for source, target in forward]
        if dim is None:
            pad = [(0, 0)] * (columns.ndim - 2) + [(0, ny - columns.shape[-1])]
            first, last = jnp.pad(columns[0], pad), jnp.pad(columns[1], pad)
        else:
            size = block.shape[dim]
            first = lax.index_in_dim(block, 0, dim, keepdims=False)
            last = lax.index_in_dim(block, size - 1, dim, keepdims=False)
        out += [lax.ppermute(last, axis, forward), lax.ppermute(first, axis, backward)]
    return out


def neighbours(ref, xlo, xhi, zlo, zhi, ylo, yhi, lead, x, centre):
    nx = ref.shape[-3]
    nz, ny = centre.shape
    sub = lax.broadcasted_iota(jnp.int32, (nz, ny), 0)
    lane = lax.broadcasted_iota(jnp.int32, (nz, ny), 1)
    prev = ref[lead + (jnp.maximum(x - 1, 0),)]
    nxt = ref[lead + (jnp.minimum(x + 1, nx - 1),)]
    xm = jnp.where(x == 0, xlo[lead], prev)
    xp = jnp.where(x == nx - 1, xhi[lead], nxt)
    zl = zlo[lead + (pl.ds(x, 1), slice(None))]
    zh = zhi[lead + (pl.ds(x, 1), slice(None))]
    zm = jnp.where(sub == 0, zl, pltpu.roll(centre, 1, 0))
    zp = jnp.where(sub == nz - 1, zh, pltpu.roll(centre, nz - 1, 0))
    yl = pltpu.roll(ylo[lead], jnp.where(x == 0, 0, ny - x), 1)
    yh = pltpu.roll(yhi[lead], ny - 1 - x, 1)
    ym = jnp.where(lane == 0, yl, pltpu.roll(centre, 1, 1))
    yp = jnp.where(lane == ny - 1, yh, pltpu.roll(centre, ny - 1, 1))
    return xm, xp, ym, yp, zm, zp


def viscosity_kernel(u, xlo, xhi, zlo, zhi, ylo, yhi, nu):
    def plane(x, carry):
        diffs = []
        for c in range(3):
            xm, xp, ym, yp, zm, zp = neighbours(u, xlo, xhi, zlo, zhi, ylo, yhi, (c,), x, u[c, x])
            diffs.append([xp - xm, yp - ym, zp - zm])
        diagonal = None
        for c in range(3):
            strain = 0.5 * diffs[c][c]
            diagonal = strain * strain if diagonal is None else diagonal + strain * strain
        cross = None
        for c in range(3):
            for d in range(c + 1, 3):
                strain = 0.25 * (diffs[c][d] + diffs[d][c])
                cross = strain * strain if cross is None else cross + strain * strain
        total = diagonal + 2.0 * cross
        nu[x] = 0.05 + 1.0 * jnp.sqrt(2.0 * total + 1e-06)
        return carry

    lax.fori_loop(0, u.shape[1], plane, 0, unroll=32)


def advance_kernel(planes, u, xlo, xhi, zlo, zhi, ylo, yhi, nu, nxlo, nxhi, nzlo, nzhi, nylo, nyhi, sent, out):
    slots = sent.shape[0]

    def plane(x, carry):
        here = nu[x]
        nxm, nxp, nym, nyp, nzm, nzp = neighbours(nu, nxlo, nxhi, nzlo, nzhi, nylo, nyhi, (), x, here)
        nu_up = [here + nxp, here + nyp, here + nzp]
        nu_low = [here + nxm, here + nym, here + nzm]
        centres = [u[c, x] for c in range(3)]
        for c in range(3):
            center = centres[c]
            xm, xp, ym, yp, zm, zp = neighbours(u, xlo, xhi, zlo, zhi, ylo, yhi, (c,), x, center)
            upper = (xp, yp, zp)
            lower = (xm, ym, zm)
            advect = None
            spread = None
            for d in range(3):
                term = centres[d] * (upper[d] - lower[d])
                flux = nu_up[d] * (upper[d] - center) - nu_low[d] * (center - lower[d])
                advect = term if advect is None else advect + term
                spread = flux if spread is None else spread + flux
            impulse = jnp.zeros_like(center)
            for s in range(slots):
                impulse = impulse + jnp.where(planes[s] == x, sent[s, c], 0.0)
            out[c, x] = center + 0.125 * (spread - advect) + impulse
        return carry

    lax.fori_loop(0, u.shape[1], plane, 0, unroll=32)


def vmem_call(kernel, out_shape, count, smem=0):
    specs = [pl.BlockSpec(memory_space=pltpu.SMEM)] * smem
    specs += [pl.BlockSpec(memory_space=pltpu.VMEM)] * (count - smem)
    return pl.pallas_call(
        kernel,
        out_shape=out_shape,
        in_specs=specs,
        out_specs=pl.BlockSpec(memory_space=pltpu.VMEM),
        interpret=INTERPRET,
    )


def stencil(velocity, planes, sent):
    u_faces = faces(velocity, 1)
    nu = vmem_call(
        viscosity_kernel, jax.ShapeDtypeStruct(velocity.shape[1:], jnp.float32), 7
    )(velocity, *u_faces)
    nu_faces = faces(nu, 0)
    return vmem_call(
        advance_kernel, jax.ShapeDtypeStruct(velocity.shape, jnp.float32), 16, smem=1
    )(planes, velocity, *u_faces, nu, *nu_faces, sent)


def body(velocity, tile_turbine, tile_plane, tile_weight, chord):
    cx = velocity.shape[1]
    vertical_coord = velocity.shape[2]
    spanwise_coord = velocity.shape[3]
    tile_count = tile_turbine.shape[3]
    actuator_count = tile_weight.shape[4]
    nturb = chord.shape[0]
    turbine_list = tile_turbine.reshape(tile_count)
    rotor_planes = tile_plane.reshape(tile_count)
    spread_weights = tile_weight.reshape(
        tile_count, actuator_count, vertical_coord * spanwise_coord
    )
    tiles = jnp.stack(
        [lax.dynamic_index_in_dim(velocity, rotor_planes[s], 1, keepdims=False) for s in range(tile_count)]
    ).reshape(tile_count, 3, vertical_coord * spanwise_coord).astype(jnp.bfloat16)
    block_local = jnp.einsum(
        "spq,scq->scp", spread_weights, tiles, preferred_element_type=jnp.float32
    )
    owning_block = (turbine_list[:, None] == jnp.arange(nturb, dtype=jnp.int32)[None, :]).astype(
        jnp.float32
    )
    partial_sample = jnp.einsum(
        "yr,yw->rw",
        owning_block,
        block_local.reshape(tile_count, -1),
        precision=lax.Precision.HIGHEST,
    )
    rows = lax.axis_size("gx")
    per_row = nturb // rows
    received = lax.all_to_all(
        partial_sample.reshape(rows, per_row, -1), "gx", split_axis=0, concat_axis=0, tiled=True
    )
    owned = jnp.sum(received, axis=0)
    for axis in ("gy", "gz"):
        count = lax.axis_size(axis)
        step = 1
        while step < count:
            pairs = [(i, i ^ step) for i in range(count)]
            owned = owned + lax.ppermute(owned, axis, pairs)
            step *= 2
    owned_coef = lax.dynamic_slice_in_dim(chord, lax.axis_index("gx") * per_row, per_row, 0)
    owned_force = actuate(owned, owned_coef)
    forces = lax.all_to_all(
        jnp.broadcast_to(owned_force[None], (rows,) + owned_force.shape),
        "gx", split_axis=0, concat_axis=0, tiled=True,
    ).reshape(nturb, -1)
    tile_force = jnp.dot(owning_block, forces, precision=lax.Precision.HIGHEST).astype(jnp.bfloat16)
    forces_sent = jnp.einsum(
        "axz,ahx->ahz",
        spread_weights,
        tile_force.reshape(tile_count, 3, actuator_count),
        preferred_element_type=jnp.float32,
    ).reshape(tile_count, 3, vertical_coord, spanwise_coord)
    predicted = stencil(velocity[:, :, :, :], rotor_planes, forces_sent)
    return (predicted, forces)


def solution(mesh):
    placed = (
        P(None, "gx", "gz", "gy"),
        P("gx", "gz", "gy", None),
        P("gx", "gz", "gy", None),
        P("gx", "gz", "gy", None, None, None),
        P(),
    )
    return jax.shard_map(
        body,
        mesh=mesh,
        in_specs=placed,
        out_specs=(P(None, "gx", "gz", "gy"), P()),
        check_vma=False,
    )
```

```python
import jax
import jax.numpy as jnp
from jax import lax
from jax.experimental import pallas as pl
from jax.experimental.pallas import tpu as pltpu
from jax.sharding import PartitionSpec as P

INTERPRET = False


def actuate(velocity_probe, coef):
    rows = velocity_probe.shape[0]
    parts = velocity_probe.reshape(rows, 3, -1)
    magnitude = jnp.sqrt(jnp.sum(parts * parts, axis=1) + 1e-06)
    return (-2.0 * coef[:, None, :] * magnitude[:, None, :] * parts).reshape(rows, -1)


def faces(block, lead):
    ny = block.shape[-1]
    if lead:
        ends = (lax.broadcasted_iota(jnp.int32, (2, ny), 1) == jnp.array([[0], [ny - 1]])).astype(jnp.float32)
        columns = jnp.einsum("cxzy,ky->kczx", block, ends, precision=lax.Precision.HIGHEST)
    else:
        lane = lax.broadcasted_iota(jnp.int32, block.shape, block.ndim - 1)
        columns = jnp.stack(
            [jnp.swapaxes(jnp.sum(jnp.where(lane == y, block, 0.0), axis=-1), -1, -2) for y in (0, ny - 1)]
        )
    out = []
    for axis, dim in (("gx", lead), ("gz", lead + 1), ("gy", None)):
        count = lax.axis_size(axis)
        forward = [(i, i + 1) for i in range(count - 1)]
        backward = [(target, source) for source, target in forward]
        if dim is None:
            pad = [(0, 0)] * (columns.ndim - 2) + [(0, ny - columns.shape[-1])]
            first, last = jnp.pad(columns[0], pad), jnp.pad(columns[1], pad)
        else:
            size = block.shape[dim]
            first = lax.index_in_dim(block, 0, dim, keepdims=False)
            last = lax.index_in_dim(block, size - 1, dim, keepdims=False)
        out += [lax.ppermute(last, axis, forward), lax.ppermute(first, axis, backward)]
    return out


def neighbours(ref, xlo, xhi, zlo, zhi, ylo, yhi, lead, x, centre):
    nx = ref.shape[-3]
    nz, ny = centre.shape
    sub = lax.broadcasted_iota(jnp.int32, (nz, ny), 0)
    lane = lax.broadcasted_iota(jnp.int32, (nz, ny), 1)
    prev = ref[lead + (jnp.maximum(x - 1, 0),)]
    nxt = ref[lead + (jnp.minimum(x + 1, nx - 1),)]
    xm = jnp.where(x == 0, xlo[lead], prev)
    xp = jnp.where(x == nx - 1, xhi[lead], nxt)
    zl = zlo[lead + (pl.ds(x, 1), slice(None))]
    zh = zhi[lead + (pl.ds(x, 1), slice(None))]
    zm = jnp.where(sub == 0, zl, pltpu.roll(centre, 1, 0))
    zp = jnp.where(sub == nz - 1, zh, pltpu.roll(centre, nz - 1, 0))
    yl = pltpu.roll(ylo[lead], jnp.where(x == 0, 0, ny - x), 1)
    yh = pltpu.roll(yhi[lead], ny - 1 - x, 1)
    ym = jnp.where(lane == 0, yl, pltpu.roll(centre, 1, 1))
    yp = jnp.where(lane == ny - 1, yh, pltpu.roll(centre, ny - 1, 1))
    return xm, xp, ym, yp, zm, zp


def viscosity_kernel(u, xlo, xhi, zlo, zhi, ylo, yhi, nu):
    def plane(x, carry):
        diffs = []
        for c in range(3):
            xm, xp, ym, yp, zm, zp = neighbours(u, xlo, xhi, zlo, zhi, ylo, yhi, (c,), x, u[c, x])
            diffs.append([xp - xm, yp - ym, zp - zm])
        diagonal = None
        for c in range(3):
            strain = 0.5 * diffs[c][c]
            diagonal = strain * strain if diagonal is None else diagonal + strain * strain
        cross = None
        for c in range(3):
            for d in range(c + 1, 3):
                strain = 0.25 * (diffs[c][d] + diffs[d][c])
                cross = strain * strain if cross is None else cross + strain * strain
        total = diagonal + 2.0 * cross
        nu[x] = 0.05 + 1.0 * jnp.sqrt(2.0 * total + 1e-06)
        return carry

    lax.fori_loop(0, u.shape[1], plane, 0, unroll=64)


def advance_kernel(planes, u, xlo, xhi, zlo, zhi, ylo, yhi, nu, nxlo, nxhi, nzlo, nzhi, nylo, nyhi, sent, out):
    slots = sent.shape[0]

    def plane(x, carry):
        here = nu[x]
        nxm, nxp, nym, nyp, nzm, nzp = neighbours(nu, nxlo, nxhi, nzlo, nzhi, nylo, nyhi, (), x, here)
        nu_up = [here + nxp, here + nyp, here + nzp]
        nu_low = [here + nxm, here + nym, here + nzm]
        centres = [u[c, x] for c in range(3)]
        for c in range(3):
            center = centres[c]
            xm, xp, ym, yp, zm, zp = neighbours(u, xlo, xhi, zlo, zhi, ylo, yhi, (c,), x, center)
            upper = (xp, yp, zp)
            lower = (xm, ym, zm)
            advect = None
            spread = None
            for d in range(3):
                term = centres[d] * (upper[d] - lower[d])
                flux = nu_up[d] * (upper[d] - center) - nu_low[d] * (center - lower[d])
                advect = term if advect is None else advect + term
                spread = flux if spread is None else spread + flux
            impulse = jnp.zeros_like(center)
            for s in range(slots):
                impulse = impulse + jnp.where(planes[s] == x, sent[s, c], 0.0)
            out[c, x] = center + 0.125 * (spread - advect) + impulse
        return carry

    lax.fori_loop(0, u.shape[1], plane, 0, unroll=64)


def vmem_call(kernel, out_shape, count, smem=0):
    specs = [pl.BlockSpec(memory_space=pltpu.SMEM)] * smem
    specs += [pl.BlockSpec(memory_space=pltpu.VMEM)] * (count - smem)
    return pl.pallas_call(
        kernel,
        out_shape=out_shape,
        in_specs=specs,
        out_specs=pl.BlockSpec(memory_space=pltpu.VMEM),
        interpret=INTERPRET,
    )


def stencil(velocity, planes, sent):
    u_faces = faces(velocity, 1)
    nu = vmem_call(
        viscosity_kernel, jax.ShapeDtypeStruct(velocity.shape[1:], jnp.float32), 7
    )(velocity, *u_faces)
    nu_faces = faces(nu, 0)
    return vmem_call(
        advance_kernel, jax.ShapeDtypeStruct(velocity.shape, jnp.float32), 16, smem=1
    )(planes, velocity, *u_faces, nu, *nu_faces, sent)


def body(velocity, tile_turbine, tile_plane, tile_weight, chord):
    cx = velocity.shape[1]
    vertical_coord = velocity.shape[2]
    spanwise_coord = velocity.shape[3]
    tile_count = tile_turbine.shape[3]
    actuator_count = tile_weight.shape[4]
    nturb = chord.shape[0]
    turbine_list = tile_turbine.reshape(tile_count)
    rotor_planes = tile_plane.reshape(tile_count)
    spread_weights = tile_weight.reshape(
        tile_count, actuator_count, vertical_coord * spanwise_coord
    )
    tiles = jnp.stack(
        [lax.dynamic_index_in_dim(velocity, rotor_planes[s], 1, keepdims=False) for s in range(tile_count)]
    ).reshape(tile_count, 3, vertical_coord * spanwise_coord).astype(jnp.bfloat16)
    block_local = jnp.einsum(
        "spq,scq->scp", spread_weights, tiles, preferred_element_type=jnp.float32
    )
    owning_block = (turbine_list[:, None] == jnp.arange(nturb, dtype=jnp.int32)[None, :]).astype(
        jnp.float32
    )
    partial_sample = jnp.einsum(
        "yr,yw->rw",
        owning_block,
        block_local.reshape(tile_count, -1),
        precision=lax.Precision.HIGHEST,
    )
    rows = lax.axis_size("gx")
    per_row = nturb // rows
    received = lax.all_to_all(
        partial_sample.reshape(rows, per_row, -1), "gx", split_axis=0, concat_axis=0, tiled=True
    )
    owned = jnp.sum(received, axis=0)
    for axis in ("gy", "gz"):
        count = lax.axis_size(axis)
        step = 1
        while step < count:
            pairs = [(i, i ^ step) for i in range(count)]
            owned = owned + lax.ppermute(owned, axis, pairs)
            step *= 2
    owned_coef = lax.dynamic_slice_in_dim(chord, lax.axis_index("gx") * per_row, per_row, 0)
    owned_force = actuate(owned, owned_coef)
    forces = lax.all_to_all(
        jnp.broadcast_to(owned_force[None], (rows,) + owned_force.shape),
        "gx", split_axis=0, concat_axis=0, tiled=True,
    ).reshape(nturb, -1)
    tile_force = jnp.dot(owning_block, forces, precision=lax.Precision.HIGHEST).astype(jnp.bfloat16)
    forces_sent = jnp.einsum(
        "axz,ahx->ahz",
        spread_weights,
        tile_force.reshape(tile_count, 3, actuator_count),
        preferred_element_type=jnp.float32,
    ).reshape(tile_count, 3, vertical_coord, spanwise_coord)
    predicted = stencil(velocity[:, :, :, :], rotor_planes, forces_sent)
    return (predicted, forces)


def solution(mesh):
    placed = (
        P(None, "gx", "gz", "gy"),
        P("gx", "gz", "gy", None),
        P("gx", "gz", "gy", None),
        P("gx", "gz", "gy", None, None, None),
        P(),
    )
    return jax.shard_map(
        body,
        mesh=mesh,
        in_specs=placed,
        out_specs=(P(None, "gx", "gz", "gy"), P()),
        check_vma=False,
    )
```
